32 devices in a mesh: node: 8 (over z, y), rep: 4 (over x, core).
Axes of the slice: x: 2, y: 2, z: 4, core: 2. Of those that a mesh axis runs over, the one named last changes fastest.
Arguments:
- coords: float32 [3, 4096], P(None, 'node'), may hold values from 0 to 2, as said below
- omega: bfloat16 [4096, 512], P('node', 'rep'), may hold values from -6 to 6
- skeleton: int32 [8, 256], P('node', 'rep'), may hold values from 0 to 4095, as said below
Outputs:
- row_sample: bfloat16 [4096, 512], P('node', 'rep')
- col_sample: float32 [4096, 512], P('node', 'rep')
The draws below stay inside these ranges and needn't reach their ends.
Inputs may be any that keep to these rules, and one draw needn't show every extreme that they name: `skeleton`: each node's list holds distinct indices, none inside its own points, at most 73 inside the points of any one other node; in every draw one node's points hold exactly 73 indices of every other node's list. `coords`: the first coordinate of point p lies between 2 (p // 512) / 8 and 2 (p // 512 + 1) / 8; the other two lie in [0, 1].
All inputs are finite; a program needn't handle non-finite values.
Results may differ from the reference program's by a relative error of at most 0.0049.
Values may be sent and summed in bfloat16 or wider, within the bound.
No kernel may reach another device: no remote copies, remote signals or barrier semaphores. Data moves between devices by JAX's collectives and lax.ppermute only.
A program may use at most 128 MiB of HBM per device.

```python
import jax
import jax.numpy as jnp
from jax import lax

LEAF = 512
RANK = 256
SAMP = 512
NPTS = 4096
N_NODE = 8


def draw_coords(key, part):
    unit = jax.random.uniform(key, (3, N_NODE * LEAF), jnp.float32)
    leaf_ids = (jnp.arange(N_NODE * LEAF) // LEAF).astype(jnp.float32)
    first = 2.0 * (leaf_ids + unit[0]) / N_NODE
    others = unit[1:]
    return jnp.concatenate([first[None, :], others], axis=0).astype(jnp.float32)


def draw_skeleton(key, part):
    key_one, random_key_second, key_three, key_four, key_five = jax.random.split(key, 5)
    capacity = max(8, 2 * RANK // (N_NODE - 1))
    position_count = N_NODE * capacity
    node_ids = jnp.arange(N_NODE, dtype=jnp.int32)
    popular = jax.random.randint(key_one, (), 0, N_NODE, dtype=jnp.int32)
    filled_owner = jnp.where(node_ids == popular, (popular + 1) % N_NODE, popular)
    linear_index = jnp.arange(position_count, dtype=jnp.int32).reshape(1, N_NODE, capacity)
    holder_preference = jax.random.randint(random_key_second, (N_NODE,), 0, 3, dtype=jnp.int32) * 512
    unadjusted_score = jax.random.randint(key_three, (N_NODE, N_NODE, capacity), 0, 1024, dtype=jnp.int32)
    owner_ids = node_ids[None, :, None]
    ranking_score = (unadjusted_score + holder_preference[None, :, None]) * position_count + linear_index
    ranking_score = jnp.where(owner_ids == filled_owner[:, None, None], 3000 * position_count + linear_index, ranking_score)
    ranking_score = jnp.where(owner_ids == node_ids[:, None, None], -1 - linear_index, ranking_score)
    unused, chosen = lax.top_k(ranking_score.reshape(N_NODE, position_count), RANK)
    chosen_owner = chosen // capacity
    chosen_slot = chosen % capacity
    offset_base = jax.random.randint(key_four, (N_NODE, N_NODE), 0, LEAF, dtype=jnp.int32)
    stride_step = 2 * jax.random.randint(key_five, (N_NODE, N_NODE), 0, LEAF // 2, dtype=jnp.int32) + 1
    base_taken = jnp.take_along_axis(offset_base, chosen_owner, axis=1)
    stride_taken = jnp.take_along_axis(stride_step, chosen_owner, axis=1)
    local_index = (base_taken + chosen_slot * stride_taken) % LEAF
    return (chosen_owner * LEAF + local_index).astype(jnp.int32)


def block_levels(rng, shape, shards, smallest, high):
    gain, own = 1.0, jax.random.fold_in(rng, 6)
    for dim, blocks in shards:
        heights = jnp.exp(jax.random.uniform(jax.random.fold_in(own, dim), (blocks,), jnp.float32, smallest / len(shards), high / len(shards)))
        gain = gain * jnp.repeat(heights, shape[dim] // blocks).reshape([-1 if axis == dim else 1 for axis in range(len(shape))])
    return gain


def centred(own_key, dims, deviation, most, cuts=(), held_as=jnp.bfloat16):
    entries = deviation * jax.random.normal(own_key, dims, jnp.float32)
    if cuts:
        entries = entries * block_levels(own_key, dims, cuts, -0.22, 0.18)
    return jnp.clip(entries, -most, most).astype(held_as)


def setup_inputs(seed: int = 0) -> dict:
    splits = jax.random.split(jax.random.key(seed), 4)
    return {
        "coords": draw_coords(jax.random.fold_in(splits[3], 71), 0),
        "omega": centred(splits[1], (NPTS, SAMP), 1.0, 6.0, ((0, 8), (1, 4))),
        "skeleton": draw_skeleton(jax.random.fold_in(splits[3], 71), 0),
    }


kernel_scale = 0.0078125
softening = 0.02

def kernel_tile(first_points, target_points):
    squared = (first_points[0][:, None] - target_points[0][None, :]) ** 2
    squared = squared + (first_points[1][:, None] - target_points[1][None, :]) ** 2
    squared = squared + (first_points[2][:, None] - target_points[2][None, :]) ** 2
    return (kernel_scale * lax.rsqrt(squared + softening * softening)).astype(jnp.bfloat16)

def reference(coords, omega, skeleton):
    padded_points = jnp.pad(coords, ((0, 0), (LEAF, LEAF)))
    padded_rows = jnp.pad(omega, ((LEAF, LEAF), (0, 0)))

    def advance(col_total, node_index):
        start = (node_index * LEAF).astype(jnp.int32)
        own_points = lax.dynamic_slice_in_dim(coords, start, LEAF, 1)
        own_rows = lax.dynamic_slice_in_dim(omega, start, LEAF, 0)
        wide_points = lax.dynamic_slice_in_dim(padded_points, start, 3 * LEAF, 1)
        wide_rows = lax.dynamic_slice_in_dim(padded_rows, start, 3 * LEAF, 0)
        row_total = jnp.dot(kernel_tile(own_points, wide_points), wide_rows, preferred_element_type=jnp.float32)
        listed = skeleton[node_index]
        skel_tile = kernel_tile(own_points, coords[:, listed])
        row_total = row_total + jnp.dot(skel_tile, omega[listed], preferred_element_type=jnp.float32)
        transposed = lax.dot_general(skel_tile, own_rows, (((0,), (0,)), ((), ())), preferred_element_type=jnp.float32)
        col_total = col_total.at[listed].add(transposed)
        return (col_total, row_total.astype(jnp.bfloat16))
    col_total, blocked_rows = lax.scan(advance, jnp.zeros((N_NODE * LEAF, SAMP), jnp.float32), jnp.arange(N_NODE, dtype=jnp.int32))
    return (blocked_rows.reshape(N_NODE * LEAF, SAMP), col_total)
```

```python
import functools

import jax
import jax.numpy as jnp
from jax import lax
from jax.experimental import pallas as pl
from jax.experimental.pallas import tpu as pltpu
from jax.sharding import PartitionSpec as P

kernel_scale = 0.0078125
softening = 0.02
stretch = 1.0 / kernel_scale
soft_term = softening * softening
TERMS = 3
LANES = 128

VMEM = pl.BlockSpec(memory_space=pltpu.VMEM)
ROOM = pltpu.CompilerParams(vmem_limit_bytes=12 * 1024 * 1024)


def place_of(node, n):
    return jnp.where(node % 2 == 0, node // 2, n - 1 - node // 2)


def node_at(place, n):
    place = lax.rem(place + n, n)
    return jnp.where(place < (n + 1) // 2, 2 * place, 2 * (n - 1 - place) + 1)


def around(distance, n):
    return node_at(place_of(lax.axis_index("node"), n) + distance, n)


def coord_rows(leaf):
    rows = 3 * TERMS * (leaf // LANES)
    return -(-rows // 16) * 16


def prep_kernel(coords_ref, omega_ref, msg_ref, wide_ref):
    leaf = coords_ref.shape[1]
    chunks = leaf // LANES
    msg_ref[0:leaf, :] = omega_ref[...]
    scaled = coords_ref[...] * stretch
    rows = []
    for c in range(3):
        rest = scaled[c : c + 1, :]
        for _ in range(TERMS):
            term = rest.astype(jnp.bfloat16).astype(jnp.float32)
            rest = rest - term
            rows += [term[:, k * LANES : (k + 1) * LANES] for k in range(chunks)]
    pad = coord_rows(leaf) - len(rows)
    rows.append(jnp.zeros((pad, LANES), jnp.float32))
    msg_ref[leaf:, :] = jnp.concatenate(rows, axis=0).astype(jnp.bfloat16)
    eight = jnp.concatenate([scaled, jnp.zeros((5, leaf), jnp.float32)], axis=0)
    columns = eight.T
    for c in range(3):
        wide_ref[c] = jnp.broadcast_to(columns[:, c : c + 1], (leaf, LANES))


def prep(coords, omega):
    leaf = coords.shape[1]
    return pl.pallas_call(
        prep_kernel,
        out_shape=(
            jax.ShapeDtypeStruct((leaf + coord_rows(leaf), LANES), jnp.bfloat16),
            jax.ShapeDtypeStruct((3, leaf, LANES), jnp.float32),
        ),
        in_specs=[VMEM, VMEM],
        out_specs=(VMEM, VMEM),
        compiler_params=ROOM,
        name="prep",
    )(coords, omega)


def block_entries(wide_ref, msg_ref, tile_ref):
    leaf = wide_ref.shape[1]
    chunks = leaf // LANES
    tail = msg_ref[leaf:, :].astype(jnp.float32)
    for k in range(chunks):
        target = []
        for c in range(3):
            row = [tail[(c * TERMS + t) * chunks + k : (c * TERMS + t) * chunks + k + 1, :] for t in range(TERMS)]
            target.append((row[0] + row[1]) + row[2])
        step = 64
        for p in range(0, leaf, step):
            squared = (wide_ref[0, p : p + step, :] - target[0]) ** 2
            squared = squared + (wide_ref[1, p : p + step, :] - target[1]) ** 2
            squared = squared + (wide_ref[2, p : p + step, :] - target[2]) ** 2
            entry = lax.rsqrt(squared + soft_term * stretch * stretch)
            tile_ref[p : p + step, k * LANES : (k + 1) * LANES] = entry.astype(jnp.bfloat16)


def count_wide(lists_ref, first, rows, start, leaf):
    points = lax.broadcasted_iota(jnp.int32, (leaf, LANES), 0) + start
    total = jnp.zeros((leaf, LANES), jnp.float32)
    hits = [
        (points == lists_ref[pl.ds(first + r, 1), :]).astype(jnp.float32).astype(jnp.bfloat16)
        for r in range(rows)
    ]
    ones = jnp.ones((LANES, LANES), jnp.bfloat16)
    for hit in hits:
        total = total + jnp.dot(hit, ones, preferred_element_type=jnp.float32)
    return total


def own_kernel(wide_ref, msg_ref, row_ref, tile_ref):
    leaf = wide_ref.shape[1]
    block_entries(wide_ref, msg_ref, tile_ref)
    row_ref[...] = jnp.dot(tile_ref[...], msg_ref[0:leaf, :], preferred_element_type=jnp.float32)


def own_block(wide, msg):
    leaf = wide.shape[1]
    return pl.pallas_call(
        own_kernel,
        out_shape=jax.ShapeDtypeStruct((leaf, LANES), jnp.float32),
        in_specs=[VMEM, VMEM],
        out_specs=VMEM,
        scratch_shapes=[pltpu.VMEM((leaf, leaf), jnp.bfloat16)],
        compiler_params=ROOM,
        name="own_block",
    )(wide, msg)


def step_kernel(n, away, list_rows, wide_ref, mine_ref, row_in_ref, *refs):
    count = len(away)
    blocks, outs = refs[:count], refs[count : 2 * count]
    row_ref, tile_ref = refs[2 * count], refs[2 * count + 1]
    leaf = wide_ref.shape[1]
    me = lax.axis_index("node")
    total = row_in_ref[...]
    for b in range(count):
        block_entries(wide_ref, blocks[b], tile_ref)
        node = around(away[b], n)
        near = jnp.where(jnp.abs(node - me) <= 1, 1.0, 0.0)
        samples = blocks[b][0:leaf, :]
        weight = count_wide(mine_ref, 0, list_rows, node * leaf, leaf) + near
        weighted = (weight * samples.astype(jnp.float32)).astype(jnp.bfloat16)
        both = jnp.dot(
            tile_ref[...], jnp.concatenate([samples, weighted], axis=1), preferred_element_type=jnp.float32
        )
        outs[b][...] = both[:, :LANES]
        total = total + both[:, LANES:]
    row_ref[...] = total


def step_blocks(n, away, wide, mine, row, blocks):
    leaf = wide.shape[1]
    count = len(blocks)
    part = jax.ShapeDtypeStruct((leaf, LANES), jnp.float32)
    outs = pl.pallas_call(
        functools.partial(step_kernel, n, away, mine.shape[0]),
        out_shape=[part] * (count + 1),
        in_specs=[VMEM] * (3 + count),
        out_specs=[VMEM] * (count + 1),
        scratch_shapes=[pltpu.VMEM((leaf, leaf), jnp.bfloat16)],
        compiler_params=ROOM,
        name="step_blocks",
    )(wide, mine, row, *blocks)
    return outs[:count], outs[count]


def last_kernel(n, away, list_rows, lists_ref, row_in_ref, *refs):
    count = len(away)
    parts, row_ref, col_ref = refs[:count], refs[count], refs[count + 1]
    leaf = row_in_ref.shape[0]
    me = lax.axis_index("node")
    row_ref[...] = row_in_ref[...].astype(row_ref.dtype)
    total = jnp.zeros_like(row_in_ref)
    for b in range(count):
        slot = around(away[b], n) ^ me
        mask = count_wide(lists_ref, slot * list_rows, list_rows, me * leaf, leaf)
        total = total + mask * parts[b][...]
    col_ref[...] = total


def finish(n, away, lists, list_rows, row, parts):
    leaf = row.shape[0]
    return pl.pallas_call(
        functools.partial(last_kernel, n, away, list_rows),
        out_shape=(
            jax.ShapeDtypeStruct((leaf, LANES), jnp.bfloat16),
            jax.ShapeDtypeStruct((leaf, LANES), jnp.float32),
        ),
        in_specs=[VMEM] * (2 + len(parts)),
        out_specs=(VMEM, VMEM),
        compiler_params=ROOM,
        name="finish",
    )(lists, row, *parts)


def swap(block, axis, bit):
    return lax.ppermute(block, axis, [(i, i ^ bit) for i in range(lax.axis_size(axis))])


def on_device(coords, omega, skeleton):
    n = lax.axis_size("node")
    reps = lax.axis_size("rep")
    cycle = list(range(0, n, 2)) + list(range(n - 1 - n % 2, 0, -2))
    hops = [(cycle[k], cycle[(k + 1) % n]) for k in range(n)]
    back = [(b, a) for a, b in hops]

    msg, wide = prep(coords, omega)
    ahead, behind = [msg], [msg]
    for s in range(1, n // 2 + 1):
        ahead.append(lax.ppermute(ahead[-1], "node", hops))
        if s < n - s:
            behind.append(lax.ppermute(behind[-1], "node", back))

    mine = skeleton
    bit = 1
    while bit < reps:
        mine = jnp.concatenate([mine, swap(mine, "rep", bit)], axis=1 if mine.shape[1] < LANES else 0)
        bit *= 2
    list_rows = mine.shape[0]
    lists = mine
    bit = 1
    while bit < n:
        lists = jnp.concatenate([lists, swap(lists, "node", bit)], axis=0)
        bit *= 2

    row = own_block(wide, msg)
    parts, away = [], []
    for s in range(1, n // 2 + 1):
        blocks, at = [ahead[s]], [-s]
        if s < n - s:
            blocks.append(behind[s])
            at.append(s)
        outs, row = step_blocks(n, at, wide, mine, row, blocks)
        parts += outs
        away += at
    return finish(n, away, lists, list_rows, row, parts)


def solution(mesh):
    in_specs = (P(None, "node"), P("node", "rep"), P("node", "rep"))
    out_specs = (P("node", "rep"), P("node", "rep"))
    return jax.shard_map(on_device, mesh=mesh, in_specs=in_specs, out_specs=out_specs, check_vma=False)
```

```python
import functools

import jax
import jax.numpy as jnp
from jax import lax
from jax.experimental import pallas as pl
from jax.experimental.pallas import tpu as pltpu
from jax.sharding import PartitionSpec as P


kernel_scale = 0.0078125
softening = 0.02
stretch = 1.0 / kernel_scale
soft_term = softening * softening * stretch * stretch
TERMS = 3
LANES = 128
BASE = 256
QUAD = (1, 2, 3)

VMEM = pl.BlockSpec(memory_space=pltpu.VMEM)
ROOM = pltpu.CompilerParams(vmem_limit_bytes=16 * 1024 * 1024)


def tail_rows(leaf, list_rows):
    rows = 3 * TERMS * (leaf // LANES)
    return -(-rows // 16) * 16 + -(-2 * list_rows // 16) * 16


def list_start(size, list_rows):
    return size - -(-2 * list_rows // 16) * 16


def prep_kernel(coords_ref, omega_ref, piece_ref, msg_ref, wide_ref, own_ref, points, sems):
    leaf = points.shape[1]
    chunks = leaf // LANES
    fetch = pltpu.make_async_copy(coords_ref, points, sems.at[0])
    block = pltpu.make_async_copy(omega_ref, msg_ref.at[pl.ds(0, leaf)], sems.at[1])
    piece = pltpu.make_async_copy(piece_ref, own_ref, sems.at[2])
    fetch.start()
    block.start()
    piece.start()
    fetch.wait()
    scaled = points[...] * stretch
    rows = []
    for c in range(3):
        rest = scaled[c : c + 1, :]
        for _ in range(TERMS):
            term = rest.astype(jnp.bfloat16).astype(jnp.float32)
            rest = rest - term
            rows += [term[:, k * LANES : (k + 1) * LANES] for k in range(chunks)]
    spare = msg_ref.shape[0] - leaf - len(rows)
    rows.append(jnp.zeros((spare, LANES), jnp.float32))
    msg_ref[leaf:, :] = jnp.concatenate(rows, axis=0).astype(jnp.bfloat16)
    columns = jnp.concatenate([scaled, jnp.zeros((5, leaf), jnp.float32)], axis=0).T
    for c in range(3):
        wide_ref[c] = jnp.broadcast_to(columns[:, c : c + 1], (leaf, LANES))
    block.wait()
    piece.wait()


def prep(list_rows, coords, omega, piece):
    leaf = coords.shape[1]
    return pl.pallas_call(
        prep_kernel,
        out_shape=(
            jax.ShapeDtypeStruct((leaf + tail_rows(leaf, list_rows), LANES), jnp.bfloat16),
            jax.ShapeDtypeStruct((3, leaf, LANES), jnp.float32),
            jax.ShapeDtypeStruct(piece.shape, piece.dtype),
        ),
        in_specs=[pl.BlockSpec(memory_space=pltpu.HBM)] * 3,
        out_specs=(VMEM,) * 3,
        scratch_shapes=[pltpu.VMEM(coords.shape, jnp.float32), pltpu.SemaphoreType.DMA((3,))],
        cost_estimate=pl.CostEstimate(flops=1000000, bytes_accessed=0, transcendentals=0),
        compiler_params=ROOM,
        name="prep",
    )(coords, omega, piece)


def attach_kernel(list_rows, msg_in_ref, *refs):
    pieces, msg_ref, tail_ref = refs[:-2], refs[-2], refs[-1]
    size, rows_all = tail_ref.shape[0], msg_ref.shape[0]
    first = list_start(rows_all, list_rows)
    listed = jnp.concatenate([piece[...] for piece in pieces], axis=1)
    rows = []
    for digit in (listed // BASE, listed % BASE):
        digit = digit.astype(jnp.float32)
        rows += [digit[:, r * LANES : (r + 1) * LANES] for r in range(list_rows)]
    rows.append(jnp.zeros((rows_all - first - len(rows), LANES), jnp.float32))
    rows = jnp.concatenate(rows, axis=0).astype(jnp.bfloat16)
    msg_ref[first:, :] = rows
    held = size - (rows_all - first)
    tail_ref[0:held, :] = msg_in_ref[rows_all - size : first, :]
    tail_ref[held:, :] = rows


def attach(list_rows, size, msg, pieces):
    return pl.pallas_call(
        functools.partial(attach_kernel, list_rows),
        out_shape=(
            jax.ShapeDtypeStruct(msg.shape, msg.dtype),
            jax.ShapeDtypeStruct((size, LANES), msg.dtype),
        ),
        in_specs=[VMEM] * (1 + len(pieces)),
        out_specs=(VMEM, VMEM),
        input_output_aliases={0: 0},
        compiler_params=ROOM,
        name="attach",
    )(msg, *pieces)


def pack_kernel(block_ref, tail_ref, msg_ref):
    leaf = block_ref.shape[0]
    msg_ref[0:leaf, :] = block_ref[...]
    msg_ref[leaf:, :] = tail_ref[...]


def pack(block, tail):
    return pl.pallas_call(
        pack_kernel,
        out_shape=jax.ShapeDtypeStruct((block.shape[0] + tail.shape[0], LANES), block.dtype),
        in_specs=[VMEM, VMEM],
        out_specs=VMEM,
        compiler_params=ROOM,
        name="pack",
    )(block, tail)


def block_entries(wide_ref, tail, tile_ref):
    leaf = wide_ref.shape[1]
    chunks = leaf // LANES
    step = 64
    for k in range(chunks):
        target = []
        for c in range(3):
            row = [(c * TERMS + t) * chunks + k for t in range(TERMS)]
            row = [tail[r : r + 1, :] for r in row]
            target.append((row[0] + row[1]) + row[2])
        for p in range(0, leaf, step):
            squared = (wide_ref[0, p : p + step, :] - target[0]) ** 2
            squared = squared + (wide_ref[1, p : p + step, :] - target[1]) ** 2
            squared = squared + (wide_ref[2, p : p + step, :] - target[2]) ** 2
            entry = lax.rsqrt(squared + soft_term)
            tile_ref[p : p + step, k * LANES : (k + 1) * LANES] = entry.astype(jnp.bfloat16)


def listed_in(tail, list_rows):
    first = list_start(tail.shape[0], list_rows)
    high = tail[first : first + list_rows, :]
    low = tail[first + list_rows : first + 2 * list_rows, :]
    return high * BASE + low


def count_wide(listed, node, leaf):
    points = lax.broadcasted_iota(jnp.int32, (leaf, LANES), 0) + node * leaf
    points = points.astype(jnp.float32)
    hits = jnp.zeros((leaf, LANES), jnp.float32)
    for r in range(listed.shape[0]):
        hits = hits + jnp.where(points == listed[r : r + 1, :], 1.0, 0.0)
    ones = jnp.ones((LANES, LANES), jnp.bfloat16)
    return jnp.dot(hits.astype(jnp.bfloat16), ones, preferred_element_type=jnp.float32)


def weight_wide(mine, node, me, leaf):
    near = jnp.where(jnp.abs(node - me) <= 1, 1.0, 0.0)
    return (count_wide(mine, node, leaf) + near).astype(jnp.bfloat16)


def both_products(tile, samples, weight):
    weighted = (weight.astype(jnp.float32) * samples.astype(jnp.float32)).astype(jnp.bfloat16)
    both = jnp.dot(tile, jnp.concatenate([samples, weighted], axis=1), preferred_element_type=jnp.float32)
    return both[:, :LANES], both[:, LANES:]


def blocks_kernel(list_rows, bits, started, wide_ref, tail_ref, *refs):
    msgs = refs[: len(bits)]
    row_ref, col_ref, tile_ref = refs[-3], refs[-2], refs[-1]
    leaf = wide_ref.shape[1]
    me = lax.axis_index("node")
    mine = listed_in(tail_ref[...].astype(jnp.float32), list_rows)
    if started:
        row_total, col_total = refs[len(bits)][...], refs[len(bits) + 1][...]
    else:
        row_total = jnp.zeros((leaf, LANES), jnp.float32)
        col_total = jnp.zeros((leaf, LANES), jnp.float32)
    for bit, msg in zip(bits, msgs):
        tail = msg[leaf:, :].astype(jnp.float32)
        block_entries(wide_ref, tail, tile_ref)
        weight = weight_wide(mine, me ^ bit, me, leaf)
        plain, taken = both_products(tile_ref[...], msg[0:leaf, :], weight)
        row_total = row_total + taken
        col_total = col_total + count_wide(listed_in(tail, list_rows), me, leaf) * plain
    row_ref[...] = row_total.astype(row_ref.dtype)
    col_ref[...] = col_total


def add_blocks(list_rows, bits, wide, tail, msgs, totals, row_type=jnp.float32):
    leaf = wide.shape[1]
    part = (leaf, LANES)
    return pl.pallas_call(
        functools.partial(blocks_kernel, list_rows, bits, bool(totals)),
        out_shape=(jax.ShapeDtypeStruct(part, row_type), jax.ShapeDtypeStruct(part, jnp.float32)),
        in_specs=[VMEM] * (2 + len(msgs) + len(totals)),
        out_specs=(VMEM, VMEM),
        scratch_shapes=[pltpu.VMEM((leaf, leaf), jnp.bfloat16)],
        compiler_params=ROOM,
        name="add_blocks",
    )(wide, tail, *msgs, *totals)


def swap(block, axis, bits):
    return lax.ppermute(block, axis, [(i, i ^ bits) for i in range(lax.axis_size(axis))])


def on_device(coords, omega, skeleton):
    nodes = lax.axis_size("node")
    reps = lax.axis_size("rep")
    leaf = coords.shape[1]
    list_rows = reps * skeleton.shape[1] // LANES
    size = tail_rows(leaf, list_rows)
    far_bits = [1 << k for k in range(2, nodes.bit_length() - 1)]

    across = [(0, omega)]
    for bit in reversed(far_bits):
        across += [(bits | bit, swap(block, "node", bit)) for bits, block in across]
    pieces = [swap(skeleton, "rep", bits) for bits in range(1, reps)]
    msg, wide, own_piece = prep(list_rows, coords, omega, skeleton)
    msg, tail = attach(list_rows, size, msg, [own_piece] + pieces)
    tails = [(0, tail)]
    for bit in reversed(far_bits):
        tails += [(bits | bit, swap(part, "node", bit)) for bits, part in tails]
    msgs = [swap(msg, "node", step) for step in QUAD]
    totals = add_blocks(list_rows, [0], wide, tail, [msg], ())
    totals = add_blocks(list_rows, QUAD, wide, tail, msgs, totals)
    for (bits, block), (_, part) in zip(across[1:], tails[1:]):
        msg = pack(block, part)
        msgs = [swap(msg, "node", step) for step in QUAD]
        totals = add_blocks(list_rows, [bits], wide, tail, [msg], totals)
        for step, msg in zip(QUAD, msgs):
            final = bits == across[-1][0] and step == QUAD[-1]
            totals = add_blocks(
                list_rows, [bits | step], wide, tail, [msg], totals, jnp.bfloat16 if final else jnp.float32
            )
    return totals


def solution(mesh):
    in_specs = (P(None, "node"), P("node", "rep"), P("node", "rep"))
    out_specs = (P("node", "rep"), P("node", "rep"))
    return jax.shard_map(on_device, mesh=mesh, in_specs=in_specs, out_specs=out_specs, check_vma=False)
```

```python
import functools

import jax
import jax.numpy as jnp
from jax import lax
from jax.experimental import pallas as pl
from jax.experimental.pallas import tpu as pltpu
from jax.sharding import PartitionSpec as P


kernel_scale = 0.0078125
softening = 0.02
stretch = 1.0 / kernel_scale
soft_term = softening * softening * stretch * stretch
TERMS = 3
LANES = 128
BASE = 256
QUAD = (1, 2, 3)

VMEM = pl.BlockSpec(memory_space=pltpu.VMEM)
ROOM = pltpu.CompilerParams(vmem_limit_bytes=16 * 1024 * 1024)


def coord_rows(leaf):
    return 3 * TERMS * (leaf // LANES)


def tail_rows(leaf, list_rows):
    return -(-(coord_rows(leaf) + 2 * list_rows) // 16) * 16


def prep_kernel(coords_ref, omega_ref, piece_ref, msg_ref, wide_ref, own_ref, points, sems):
    leaf = points.shape[1]
    chunks = leaf // LANES
    fetch = pltpu.make_async_copy(coords_ref, points, sems.at[0])
    block = pltpu.make_async_copy(omega_ref, msg_ref.at[pl.ds(0, leaf)], sems.at[1])
    piece = pltpu.make_async_copy(piece_ref, own_ref, sems.at[2])
    fetch.start()
    block.start()
    piece.start()
    fetch.wait()
    scaled = points[...] * stretch
    rows = []
    for c in range(3):
        rest = scaled[c : c + 1, :]
        for _ in range(TERMS):
            term = rest.astype(jnp.bfloat16).astype(jnp.float32)
            rest = rest - term
            rows += [term[:, k * LANES : (k + 1) * LANES] for k in range(chunks)]
    spare = msg_ref.shape[0] - leaf - len(rows)
    rows.append(jnp.zeros((spare, LANES), jnp.float32))
    msg_ref[leaf:, :] = jnp.concatenate(rows, axis=0).astype(jnp.bfloat16)
    columns = jnp.concatenate([scaled, jnp.zeros((5, leaf), jnp.float32)], axis=0).T
    for c in range(3):
        wide_ref[c] = jnp.broadcast_to(columns[:, c : c + 1], (leaf, LANES))
    block.wait()
    piece.wait()


def prep(list_rows, coords, omega, piece):
    leaf = coords.shape[1]
    return pl.pallas_call(
        prep_kernel,
        out_shape=(
            jax.ShapeDtypeStruct((leaf + tail_rows(leaf, list_rows), LANES), jnp.bfloat16),
            jax.ShapeDtypeStruct((3, leaf, LANES), jnp.float32),
            jax.ShapeDtypeStruct(piece.shape, piece.dtype),
        ),
        in_specs=[pl.BlockSpec(memory_space=pltpu.HBM)] * 3,
        out_specs=(VMEM,) * 3,
        scratch_shapes=[pltpu.VMEM(coords.shape, jnp.float32), pltpu.SemaphoreType.DMA((3,))],
        cost_estimate=pl.CostEstimate(flops=1000000, bytes_accessed=0, transcendentals=0),
        compiler_params=ROOM,
        name="prep",
    )(*[pltpu.with_memory_space_constraint(x, pltpu.HBM) for x in (coords, omega, piece)])


def attach_kernel(list_rows, msg_in_ref, *refs):
    pieces, msg_ref, tail_ref = refs[:-2], refs[-2], refs[-1]
    leaf = msg_ref.shape[0] - tail_ref.shape[0]
    first = coord_rows(leaf)
    listed = jnp.concatenate([piece[...] for piece in pieces], axis=1)
    rows = []
    for digit in (listed // BASE, listed % BASE):
        digit = digit.astype(jnp.float32)
        rows += [digit[:, r * LANES : (r + 1) * LANES] for r in range(list_rows)]
    tail = msg_in_ref[leaf:, :].astype(jnp.float32)
    rows = [tail[:first, :]] + rows + [tail[first + 2 * list_rows :, :]]
    tail = jnp.concatenate([part for part in rows if part.shape[0]], axis=0).astype(jnp.bfloat16)
    msg_ref[leaf:, :] = tail
    tail_ref[...] = tail


def attach(list_rows, size, msg, pieces):
    return pl.pallas_call(
        functools.partial(attach_kernel, list_rows),
        out_shape=(
            jax.ShapeDtypeStruct(msg.shape, msg.dtype),
            jax.ShapeDtypeStruct((size, LANES), msg.dtype),
        ),
        in_specs=[VMEM] * (1 + len(pieces)),
        out_specs=(VMEM, VMEM),
        input_output_aliases={0: 0},
        compiler_params=ROOM,
        name="attach",
    )(msg, *pieces)


def pack_kernel(block_ref, tail_ref, msg_ref):
    leaf = block_ref.shape[0]
    msg_ref[0:leaf, :] = block_ref[...]
    msg_ref[leaf:, :] = tail_ref[...]


def pack(block, tail):
    return pl.pallas_call(
        pack_kernel,
        out_shape=jax.ShapeDtypeStruct((block.shape[0] + tail.shape[0], LANES), block.dtype),
        in_specs=[VMEM, VMEM],
        out_specs=VMEM,
        compiler_params=ROOM,
        name="pack",
    )(block, tail)


def block_entries(wide_ref, tail, tile_ref):
    leaf = wide_ref.shape[1]
    chunks = leaf // LANES
    step = 64
    for k in range(chunks):
        target = []
        for c in range(3):
            row = [(c * TERMS + t) * chunks + k for t in range(TERMS)]
            row = [tail[r : r + 1, :] for r in row]
            target.append((row[0] + row[1]) + row[2])
        for p in range(0, leaf, step):
            squared = (wide_ref[0, p : p + step, :] - target[0]) ** 2
            squared = squared + (wide_ref[1, p : p + step, :] - target[1]) ** 2
            squared = squared + (wide_ref[2, p : p + step, :] - target[2]) ** 2
            entry = lax.rsqrt(squared + soft_term)
            tile_ref[p : p + step, k * LANES : (k + 1) * LANES] = entry.astype(jnp.bfloat16)


def listed_in(tail, leaf, list_rows):
    first = coord_rows(leaf)
    high = tail[first : first + list_rows, :]
    low = tail[first + list_rows : first + 2 * list_rows, :]
    return high * BASE + low


def count_wide(listed, node, leaf):
    points = lax.broadcasted_iota(jnp.int32, (leaf, LANES), 0) + node * leaf
    points = points.astype(jnp.float32)
    hits = jnp.zeros((leaf, LANES), jnp.float32)
    for r in range(listed.shape[0]):
        hits = hits + jnp.where(points == listed[r : r + 1, :], 1.0, 0.0)
    ones = jnp.ones((LANES, LANES), jnp.bfloat16)
    return jnp.dot(hits.astype(jnp.bfloat16), ones, preferred_element_type=jnp.float32)


def weight_wide(mine, node, me, leaf):
    near = jnp.where(jnp.abs(node - me) <= 1, 1.0, 0.0)
    return (count_wide(mine, node, leaf) + near).astype(jnp.bfloat16)


def both_products(tile, samples, weight):
    weighted = (weight.astype(jnp.float32) * samples.astype(jnp.float32)).astype(jnp.bfloat16)
    both = jnp.dot(tile, jnp.concatenate([samples, weighted], axis=1), preferred_element_type=jnp.float32)
    return both[:, :LANES], both[:, LANES:]


def blocks_kernel(list_rows, bits, started, wide_ref, tail_ref, *refs):
    msgs = refs[: len(bits)]
    row_ref, col_ref, tile_ref = refs[-3], refs[-2], refs[-1]
    leaf = wide_ref.shape[1]
    me = lax.axis_index("node")
    mine = listed_in(tail_ref[...].astype(jnp.float32), leaf, list_rows)
    if started:
        row_total, col_total = refs[len(bits)][...], refs[len(bits) + 1][...]
    else:
        row_total = jnp.zeros((leaf, LANES), jnp.float32)
        col_total = jnp.zeros((leaf, LANES), jnp.float32)
    for bit, msg in zip(bits, msgs):
        tail = msg[leaf:, :].astype(jnp.float32)
        block_entries(wide_ref, tail, tile_ref)
        weight = weight_wide(mine, me ^ bit, me, leaf)
        plain, taken = both_products(tile_ref[...], msg[0:leaf, :], weight)
        row_total = row_total + taken
        col_total = col_total + count_wide(listed_in(tail, leaf, list_rows), me, leaf) * plain
    row_ref[...] = row_total.astype(row_ref.dtype)
    col_ref[...] = col_total


def add_blocks(list_rows, bits, wide, tail, msgs, totals, row_type=jnp.float32):
    leaf = wide.shape[1]
    part = (leaf, LANES)
    return pl.pallas_call(
        functools.partial(blocks_kernel, list_rows, bits, bool(totals)),
        out_shape=(jax.ShapeDtypeStruct(part, row_type), jax.ShapeDtypeStruct(part, jnp.float32)),
        in_specs=[VMEM] * (2 + len(msgs) + len(totals)),
        out_specs=(VMEM, VMEM),
        scratch_shapes=[pltpu.VMEM((leaf, leaf), jnp.bfloat16)],
        compiler_params=ROOM,
        name="add_blocks",
    )(wide, tail, *msgs, *totals)


def swap(block, axis, bits):
    return lax.ppermute(block, axis, [(i, i ^ bits) for i in range(lax.axis_size(axis))])


def on_device(coords, omega, skeleton):
    nodes = lax.axis_size("node")
    reps = lax.axis_size("rep")
    leaf = coords.shape[1]
    list_rows = reps * skeleton.shape[1] // LANES
    size = tail_rows(leaf, list_rows)
    far_bits = [1 << k for k in range(2, nodes.bit_length() - 1)]

    across = [(0, omega)]
    for bit in reversed(far_bits):
        across += [(bits | bit, swap(block, "node", bit)) for bits, block in across]
    pieces = [swap(skeleton, "rep", bits) for bits in reversed(range(1, reps))]
    msg, wide, own_piece = prep(list_rows, coords, omega, skeleton)
    msg, tail = attach(list_rows, size, msg, [own_piece] + pieces)
    tails = [(0, tail)]
    for bit in reversed(far_bits):
        tails += [(bits | bit, swap(part, "node", bit)) for bits, part in tails]
    msgs = [swap(msg, "node", step) for step in QUAD]
    arrived = [(step, msg) for step, msg in zip(QUAD, msgs)]
    early = [(0, msg)]
    late = []
    for (bits, block), (_, part) in zip(across[1:], tails[1:]):
        msg = pack(block, part)
        late += [(bits | step, swap(msg, "node", step)) for step in QUAD]
        early.append((bits, msg))
    totals = ()
    blocks = early + arrived[2:] + arrived[:2] + late
    for place, (bits, msg) in enumerate(blocks):
        row_type = jnp.float32 if place + 1 < len(blocks) else jnp.bfloat16
        totals = add_blocks(list_rows, [bits], wide, tail, [msg], totals, row_type)
    return totals


def solution(mesh):
    in_specs = (P(None, "node"), P("node", "rep"), P("node", "rep"))
    out_specs = (P("node", "rep"), P("node", "rep"))
    return jax.shard_map(on_device, mesh=mesh, in_specs=in_specs, out_specs=out_specs, check_vma=False)
```

```python
import functools

import jax
import jax.numpy as jnp
from jax import lax
from jax.experimental import pallas as pl
from jax.experimental.pallas import tpu as pltpu
from jax.sharding import PartitionSpec as P


kernel_scale = 0.0078125
softening = 0.02
stretch = 1.0 / kernel_scale
soft_term = softening * softening * stretch * stretch
TERMS = 3
LANES = 128
BASE = 256
QUAD = (1, 2, 3)

VMEM = pl.BlockSpec(memory_space=pltpu.VMEM)
ROOM = pltpu.CompilerParams(vmem_limit_bytes=16 * 1024 * 1024)


def term_rows(leaf):
    return -(-4 * (leaf // LANES) // 16) * 16


def spare_row(leaf, index):
    chunks = leaf // LANES
    return (index // chunks) * term_rows(leaf) + 4 * (index % chunks) + 3


def split(value):
    terms = []
    for _ in range(TERMS):
        term = value.astype(jnp.bfloat16).astype(jnp.float32)
        value = value - term
        terms.append(term)
    return terms


def row_kind(rows):
    return lax.broadcasted_iota(jnp.int32, (rows, LANES), 0) % 4


def centred(points, nodes, me):
    kind = row_kind(points.shape[0])
    first = (2 * me + 1).astype(jnp.float32) * (stretch / nodes)
    middle = jnp.where(kind == 0, first, 0.5 * stretch)
    return jnp.where(kind == 3, 0.0, points - middle)


def factors(points, left):
    spare = row_kind(points.shape[0]) == 3
    square = points * points
    norm = pltpu.roll(square, 1, 0) + pltpu.roll(square, 2, 0) + pltpu.roll(square, 3, 0)
    norm = jnp.where(spare, norm + soft_term if left else norm, 0.0)
    one = jnp.where(spare, 1.0, 0.0)
    high, middle, low = split(-2.0 * points if left else points)
    norms = split(norm)
    if left:
        groups = [high + norms[0], high + norms[1], middle + norms[2], middle + one, high + one, low + one, middle, low]
    else:
        groups = [high + one, middle + one, high + one, middle + norms[0], low + norms[1], high + norms[2], low, middle]
    return groups


def chunk_of(groups, k):
    return jnp.concatenate([group[4 * k : 4 * k + 4, :] for group in groups], axis=0)


def prep_kernel(nodes, coords_ref, omega_ref, piece_ref, msg_ref, left_ref, own_ref, points, sems):
    leaf = points.shape[1]
    chunks = leaf // LANES
    fetch = pltpu.make_async_copy(coords_ref, points, sems.at[0])
    block = pltpu.make_async_copy(omega_ref, msg_ref.at[pl.ds(0, leaf)], sems.at[1])
    piece = pltpu.make_async_copy(piece_ref, own_ref, sems.at[2])
    fetch.start()
    block.start()
    piece.start()
    fetch.wait()
    scaled = points[...] * stretch
    blank = jnp.zeros((1, LANES), jnp.float32)
    rows = []
    for k in range(chunks):
        rows += [scaled[c : c + 1, k * LANES : (k + 1) * LANES] for c in range(3)] + [blank]
    rows += [blank] * (term_rows(leaf) - len(rows))
    rows = jnp.concatenate(rows, axis=0)
    msg_ref[leaf:, :] = jnp.concatenate(split(rows), axis=0).astype(jnp.bfloat16)
    groups = factors(centred(rows, nodes, lax.axis_index("node")), True)
    for k in range(chunks):
        left_ref[k * LANES : (k + 1) * LANES, :] = chunk_of(groups, k).T.astype(jnp.bfloat16)
    block.wait()
    piece.wait()


def prep(coords, omega, piece):
    leaf = coords.shape[1]
    operands = [pltpu.with_memory_space_constraint(x, pltpu.HBM) for x in (coords, omega, piece)]
    return pl.pallas_call(
        functools.partial(prep_kernel, lax.axis_size("node")),
        out_shape=(
            jax.ShapeDtypeStruct((leaf + TERMS * term_rows(leaf), LANES), jnp.bfloat16),
            jax.ShapeDtypeStruct((leaf, 32), jnp.bfloat16),
            jax.ShapeDtypeStruct(piece.shape, piece.dtype),
        ),
        in_specs=[pl.BlockSpec(memory_space=pltpu.HBM)] * 3,
        out_specs=(VMEM,) * 3,
        scratch_shapes=[pltpu.VMEM(coords.shape, jnp.float32), pltpu.SemaphoreType.DMA((3,))],
        compiler_params=ROOM,
        name="prep",
    )(*operands)


def attach_kernel(list_rows, msg_in_ref, *refs):
    pieces, msg_ref, tail_ref = refs[:-2], refs[-2], refs[-1]
    leaf = msg_ref.shape[0] - tail_ref.shape[0]
    listed = jnp.concatenate([piece[...] for piece in pieces], axis=1)
    tail = msg_in_ref[leaf:, :].astype(jnp.float32)
    place = lax.broadcasted_iota(jnp.int32, tail.shape, 0)
    index = 0
    for digit in (listed // BASE, listed % BASE):
        digit = digit.astype(jnp.float32)
        for r in range(list_rows):
            tail = jnp.where(place == spare_row(leaf, index), digit[:, r * LANES : (r + 1) * LANES], tail)
            index += 1
    tail = tail.astype(jnp.bfloat16)
    msg_ref[leaf:, :] = tail
    tail_ref[...] = tail


def attach(list_rows, msg, pieces, leaf):
    return pl.pallas_call(
        functools.partial(attach_kernel, list_rows),
        out_shape=(
            jax.ShapeDtypeStruct(msg.shape, msg.dtype),
            jax.ShapeDtypeStruct((msg.shape[0] - leaf, LANES), msg.dtype),
        ),
        in_specs=[VMEM] * (1 + len(pieces)),
        out_specs=(VMEM, VMEM),
        input_output_aliases={0: 0},
        compiler_params=ROOM,
        name="attach",
    )(msg, *pieces)


def pack_kernel(block_ref, tail_ref, msg_ref):
    leaf = block_ref.shape[0]
    msg_ref[0:leaf, :] = block_ref[...]
    msg_ref[leaf:, :] = tail_ref[...]


def pack(block, tail):
    return pl.pallas_call(
        pack_kernel,
        out_shape=jax.ShapeDtypeStruct((block.shape[0] + tail.shape[0], LANES), block.dtype),
        in_specs=[VMEM, VMEM],
        out_specs=VMEM,
        compiler_params=ROOM,
        name="pack",
    )(block, tail)


def listed_in(tail, leaf, list_rows):
    digits = [tail[spare_row(leaf, r) : spare_row(leaf, r) + 1, :] for r in range(2 * list_rows)]
    return [digits[r] * BASE + digits[list_rows + r] for r in range(list_rows)]


def count_table(listed, first, rows):
    total = jnp.zeros((rows, LANES), jnp.float32)
    for index in listed:
        row = jnp.floor(index * (1.0 / LANES))
        column = index - row * LANES
        rows_hit = jnp.where(lax.broadcasted_iota(jnp.int32, (rows, LANES), 0).astype(jnp.float32) + first == row, 1.0, 0.0)
        lanes_hit = jnp.where(lax.broadcasted_iota(jnp.int32, (LANES, LANES), 0).astype(jnp.float32) == column, 1.0, 0.0)
        total = total + lax.dot_general(
            rows_hit.astype(jnp.bfloat16),
            lanes_hit.astype(jnp.bfloat16),
            (((1,), (1,)), ((), ())),
            preferred_element_type=jnp.float32,
        )
    return total


def widened(table):
    rows = table.shape[0]
    if rows % 8:
        table = jnp.concatenate([table, jnp.zeros((8 - rows % 8, LANES), jnp.float32)], axis=0)
    columns = table.T
    return jnp.concatenate([jnp.broadcast_to(columns[:, k : k + 1], (LANES, LANES)) for k in range(rows)], axis=0)


def block_kernel(nodes, list_rows, bits, started, left_ref, tail_ref, msg_ref, *refs):
    row_ref, col_ref, table_out_ref, right_ref, tile_ref = refs[-5:]
    leaf = left_ref.shape[0]
    chunks = leaf // LANES
    me = lax.axis_index("node")
    if started:
        row_in_ref, col_in_ref, table_ref = refs[:3]
    else:
        mine = listed_in(tail_ref[...].astype(jnp.float32), leaf, list_rows)
        table_out_ref[...] = count_table(mine, 0.0, table_out_ref.shape[0])
        table_ref = table_out_ref
    tail = msg_ref[leaf:, :].astype(jnp.float32)
    term = term_rows(leaf)
    points = (tail[0:term, :] + tail[term : 2 * term, :]) + tail[2 * term : 3 * term, :]
    groups = factors(centred(points, nodes, me), False)
    for k in range(chunks):
        right_ref[:, k * LANES : (k + 1) * LANES] = chunk_of(groups, k).astype(jnp.bfloat16)
    step = LANES
    for p in range(0, leaf, step):
        squared = jnp.dot(left_ref[p : p + step, :], right_ref[...], preferred_element_type=jnp.float32)
        tile_ref[p : p + step, :] = lax.rsqrt(squared).astype(jnp.bfloat16)
    node = me ^ bits
    near = jnp.where(jnp.abs(node - me) <= 1, 1.0, 0.0)
    samples = msg_ref[0:leaf, :]
    weight = widened(table_ref[pl.ds(node * chunks, chunks), :]) + near
    weighted = weight.astype(jnp.bfloat16) * samples
    first = (me * chunks).astype(jnp.float32)
    named = count_table(listed_in(tail, leaf, list_rows), first, -(-chunks // 8) * 8)
    mask = widened(named[0:chunks, :])
    both = jnp.dot(tile_ref[...], jnp.concatenate([samples, weighted], axis=1), preferred_element_type=jnp.float32)
    row, col = both[:, LANES:], mask * both[:, :LANES]
    if started:
        row, col = row_in_ref[...] + row, col_in_ref[...] + col
    row_ref[...] = row.astype(row_ref.dtype)
    col_ref[...] = col


def add_block(list_rows, bits, left, tail, msg, totals, row_type=jnp.float32):
    leaf = left.shape[0]
    nodes = lax.axis_size("node")
    part = (leaf, LANES)
    outs = [jax.ShapeDtypeStruct(part, row_type), jax.ShapeDtypeStruct(part, jnp.float32)]
    scratch = [pltpu.VMEM((32, leaf), jnp.bfloat16), pltpu.VMEM((leaf, leaf), jnp.bfloat16)]
    table_shape = (-(-nodes * (leaf // LANES) // 8) * 8, LANES)
    if totals:
        scratch = [pltpu.VMEM((8, LANES), jnp.float32)] + scratch
    else:
        outs.append(jax.ShapeDtypeStruct(table_shape, jnp.float32))
    result = pl.pallas_call(
        functools.partial(block_kernel, nodes, list_rows, bits, bool(totals)),
        out_shape=outs,
        in_specs=[VMEM] * (3 + len(totals)),
        out_specs=[VMEM] * len(outs),
        scratch_shapes=scratch,
        compiler_params=ROOM,
        name="add_block",
    )(left, tail, msg, *totals)
    return (result[0], result[1], totals[2] if totals else result[2])


def swap(block, axis, bits):
    return lax.ppermute(block, axis, [(i, i ^ bits) for i in range(lax.axis_size(axis))])


def on_device(coords, omega, skeleton):
    nodes = lax.axis_size("node")
    reps = lax.axis_size("rep")
    list_rows = reps * skeleton.shape[1] // LANES
    far_bits = [1 << k for k in range(2, nodes.bit_length() - 1)]

    across = [(0, omega)]
    for bit in reversed(far_bits):
        across += [(bits | bit, swap(block, "node", bit)) for bits, block in across]
    pieces = [swap(skeleton, "rep", bits) for bits in reversed(range(1, reps))]
    msg, left, own_piece = prep(coords, omega, skeleton)
    msg, tail = attach(list_rows, msg, [own_piece] + pieces, coords.shape[1])
    tails = [(0, tail)]
    for bit in reversed(far_bits):
        tails += [(bits | bit, swap(part, "node", bit)) for bits, part in tails]
    msgs = [swap(msg, "node", step) for step in QUAD]
    arrived = [(step, msg) for step, msg in zip(QUAD, msgs)]
    early = [(0, msg)]
    late = []
    for (bits, block), (_, part) in zip(across[1:], tails[1:]):
        msg = pack(block, part)
        late += [(bits | step, swap(msg, "node", step)) for step in QUAD]
        early.append((bits, msg))
    totals = ()
    blocks = early + arrived[2:] + arrived[:2] + late
    for place, (bits, msg) in enumerate(blocks):
        row_type = jnp.float32 if place + 1 < len(blocks) else jnp.bfloat16
        totals = add_block(list_rows, bits, left, tail, msg, totals, row_type)
    return totals[:2]


def solution(mesh):
    in_specs = (P(None, "node"), P("node", "rep"), P("node", "rep"))
    out_specs = (P("node", "rep"), P("node", "rep"))
    return jax.shard_map(on_device, mesh=mesh, in_specs=in_specs, out_specs=out_specs, check_vma=False)
```

```python
import functools

import jax
import jax.numpy as jnp
from jax import lax
from jax.experimental import pallas as pl
from jax.experimental.pallas import tpu as pltpu
from jax.sharding import PartitionSpec as P


kernel_scale = 0.0078125
softening = 0.02
stretch = 1.0 / kernel_scale
soft_term = softening * softening * stretch * stretch
TERMS = 3
LANES = 128
BASE = 256
QUAD = (1, 2, 3)

VMEM = pl.BlockSpec(memory_space=pltpu.VMEM)
ROOM = pltpu.CompilerParams(vmem_limit_bytes=16 * 1024 * 1024)


def term_rows(leaf):
    return -(-4 * (leaf // LANES) // 16) * 16


def spare_row(leaf, index):
    chunks = leaf // LANES
    return (index // chunks) * term_rows(leaf) + 4 * (index % chunks) + 3


def split(value):
    terms = []
    for _ in range(TERMS):
        term = value.astype(jnp.bfloat16).astype(jnp.float32)
        value = value - term
        terms.append(term)
    return terms


def row_kind(rows):
    return lax.broadcasted_iota(jnp.int32, (rows, LANES), 0) % 4


def centred(points, nodes, me):
    kind = row_kind(points.shape[0])
    first = (2 * me + 1).astype(jnp.float32) * (stretch / nodes)
    middle = jnp.where(kind == 0, first, 0.5 * stretch)
    return jnp.where(kind == 3, 0.0, points - middle)


def factors(points, left):
    spare = row_kind(points.shape[0]) == 3
    square = points * points
    norm = pltpu.roll(square, 1, 0) + pltpu.roll(square, 2, 0) + pltpu.roll(square, 3, 0)
    norm = jnp.where(spare, norm + soft_term if left else norm, 0.0)
    one = jnp.where(spare, 1.0, 0.0)
    high, middle, low = split(-2.0 * points if left else points)
    norms = split(norm)
    if left:
        groups = [high + norms[0], high + norms[1], middle + norms[2], middle + one, high + one, low + one, middle, low]
    else:
        groups = [high + one, middle + one, high + one, middle + norms[0], low + norms[1], high + norms[2], low, middle]
    return groups


def chunk_of(groups, k):
    return jnp.concatenate([group[4 * k : 4 * k + 4, :] for group in groups], axis=0)


def prep_kernel(nodes, coords_ref, omega_ref, piece_ref, msg_ref, left_ref, own_ref, points, sems):
    leaf = points.shape[1]
    chunks = leaf // LANES
    fetch = pltpu.make_async_copy(coords_ref, points, sems.at[0])
    block = pltpu.make_async_copy(omega_ref, msg_ref.at[pl.ds(0, leaf)], sems.at[1])
    piece = pltpu.make_async_copy(piece_ref, own_ref, sems.at[2])
    fetch.start()
    block.start()
    piece.start()
    fetch.wait()
    scaled = points[...] * stretch
    blank = jnp.zeros((1, LANES), jnp.float32)
    rows = []
    for k in range(chunks):
        rows += [scaled[c : c + 1, k * LANES : (k + 1) * LANES] for c in range(3)] + [blank]
    rows += [blank] * (term_rows(leaf) - len(rows))
    rows = jnp.concatenate(rows, axis=0)
    msg_ref[leaf:, :] = jnp.concatenate(split(rows), axis=0).astype(jnp.bfloat16)
    groups = factors(centred(rows, nodes, lax.axis_index("node")), True)
    for k in range(chunks):
        left_ref[k * LANES : (k + 1) * LANES, :] = chunk_of(groups, k).T.astype(jnp.bfloat16)
    block.wait()
    piece.wait()


def prep(coords, omega, piece):
    leaf = coords.shape[1]
    operands = [pltpu.with_memory_space_constraint(x, pltpu.HBM) for x in (coords, omega, piece)]
    return pl.pallas_call(
        functools.partial(prep_kernel, lax.axis_size("node")),
        out_shape=(
            jax.ShapeDtypeStruct((leaf + TERMS * term_rows(leaf), LANES), jnp.bfloat16),
            jax.ShapeDtypeStruct((leaf, 32), jnp.bfloat16),
            jax.ShapeDtypeStruct(piece.shape, piece.dtype),
        ),
        in_specs=[pl.BlockSpec(memory_space=pltpu.HBM)] * 3,
        out_specs=(VMEM,) * 3,
        scratch_shapes=[pltpu.VMEM(coords.shape, jnp.float32), pltpu.SemaphoreType.DMA((3,))],
        compiler_params=ROOM,
        name="prep",
    )(*operands)


def attach_kernel(list_rows, msg_in_ref, *refs):
    pieces, msg_ref, tail_ref = refs[:-2], refs[-2], refs[-1]
    leaf = msg_ref.shape[0] - tail_ref.shape[0]
    listed = jnp.concatenate([piece[...] for piece in pieces], axis=1)
    tail = msg_in_ref[leaf:, :].astype(jnp.float32)
    place = lax.broadcasted_iota(jnp.int32, tail.shape, 0)
    index = 0
    for digit in (listed // BASE, listed % BASE):
        digit = digit.astype(jnp.float32)
        for r in range(list_rows):
            tail = jnp.where(place == spare_row(leaf, index), digit[:, r * LANES : (r + 1) * LANES], tail)
            index += 1
    tail = tail.astype(jnp.bfloat16)
    msg_ref[0:leaf, :] = msg_in_ref[0:leaf, :]
    msg_ref[leaf:, :] = tail
    tail_ref[...] = tail


def attach(list_rows, msg, pieces, leaf):
    return pl.pallas_call(
        functools.partial(attach_kernel, list_rows),
        out_shape=(
            jax.ShapeDtypeStruct(msg.shape, msg.dtype),
            jax.ShapeDtypeStruct((msg.shape[0] - leaf, LANES), msg.dtype),
        ),
        in_specs=[VMEM] * (1 + len(pieces)),
        out_specs=(VMEM, VMEM),
        compiler_params=ROOM,
        name="attach",
    )(msg, *pieces)


def pack_kernel(list_rows, block_ref, tail_ref, own_ref, msg_ref):
    leaf = block_ref.shape[0]
    msg_ref[0:leaf, :] = block_ref[...]
    tail, own = tail_ref[...].astype(jnp.float32), own_ref[...].astype(jnp.float32)
    place = lax.broadcasted_iota(jnp.int32, tail.shape, 0)
    for r in range(2 * list_rows):
        held = spare_row(leaf, r)
        tail = jnp.where(place == spare_row(leaf, 2 * list_rows + r), own[held : held + 1, :], tail)
    msg_ref[leaf:, :] = tail.astype(jnp.bfloat16)


def pack(list_rows, block, tail, own):
    return pl.pallas_call(
        functools.partial(pack_kernel, list_rows),
        out_shape=jax.ShapeDtypeStruct((block.shape[0] + tail.shape[0], LANES), block.dtype),
        in_specs=[VMEM] * 3,
        out_specs=VMEM,
        compiler_params=ROOM,
        name="pack",
    )(block, tail, own)


def listed_in(tail, leaf, list_rows, slot=0):
    places = [spare_row(leaf, 2 * list_rows * slot + r) for r in range(2 * list_rows)]
    digits = [tail[place : place + 1, :] for place in places]
    return [digits[r] * BASE + digits[list_rows + r] for r in range(list_rows)]


def count_table(listed, first, rows):
    total = jnp.zeros((rows, LANES), jnp.float32)
    for index in listed:
        row = jnp.floor(index * (1.0 / LANES))
        column = index - row * LANES
        rows_hit = jnp.where(lax.broadcasted_iota(jnp.int32, (rows, LANES), 0).astype(jnp.float32) + first == row, 1.0, 0.0)
        lanes_hit = jnp.where(lax.broadcasted_iota(jnp.int32, (LANES, LANES), 0).astype(jnp.float32) == column, 1.0, 0.0)
        total = total + lax.dot_general(
            rows_hit.astype(jnp.bfloat16),
            lanes_hit.astype(jnp.bfloat16),
            (((1,), (1,)), ((), ())),
            preferred_element_type=jnp.float32,
        )
    return total


def widened(table):
    rows = table.shape[0]
    if rows % 8:
        table = jnp.concatenate([table, jnp.zeros((8 - rows % 8, LANES), jnp.float32)], axis=0)
    columns = table.T
    return jnp.concatenate([jnp.broadcast_to(columns[:, k : k + 1], (LANES, LANES)) for k in range(rows)], axis=0)


def block_kernel(nodes, list_rows, bits, started, masked, waiting, *refs):
    left_ref, tail_ref, msg_ref = refs[:3]
    right_ref, tile_ref = refs[-2:]
    leaf = left_ref.shape[0]
    chunks = leaf // LANES
    me = lax.axis_index("node")
    first = (me * chunks).astype(jnp.float32)
    if started:
        row_in_ref, col_in_ref, table_ref = refs[3:6]
        outs = refs[6 + waiting : -2]
    else:
        outs = refs[3:-2]
        mine = listed_in(tail_ref[...].astype(jnp.float32), leaf, list_rows)
        table_ref = outs[2]
        table_ref[...] = count_table(mine, 0.0, table_ref.shape[0])
    tail = msg_ref[leaf:, :].astype(jnp.float32)
    term = term_rows(leaf)
    points = (tail[0:term, :] + tail[term : 2 * term, :]) + tail[2 * term : 3 * term, :]
    groups = factors(centred(points, nodes, me), False)
    for k in range(chunks):
        right_ref[:, k * LANES : (k + 1) * LANES] = chunk_of(groups, k).astype(jnp.bfloat16)
    for p in range(0, leaf, LANES):
        squared = jnp.dot(left_ref[p : p + LANES, :], right_ref[...], preferred_element_type=jnp.float32)
        tile_ref[p : p + LANES, :] = lax.rsqrt(squared).astype(jnp.bfloat16)
    node = me ^ bits
    near = jnp.where(jnp.abs(node - me) <= 1, 1.0, 0.0)
    samples = msg_ref[0:leaf, :]
    weight = widened(table_ref[pl.ds(node * chunks, chunks), :]) + near
    weighted = weight.astype(jnp.bfloat16) * samples
    both = jnp.dot(tile_ref[...], jnp.concatenate([samples, weighted], axis=1), preferred_element_type=jnp.float32)
    row, col = both[:, LANES:], both[:, :LANES]
    if started:
        row = row_in_ref[...] + row
    outs[0][...] = row.astype(outs[0].dtype)
    if not masked:
        outs[1][...] = col
        return
    table_rows = -(-chunks // 8) * 8
    named = count_table(listed_in(tail, leaf, list_rows), first, table_rows)
    col = widened(named[0:chunks, :]) * col
    if started:
        col = col_in_ref[...] + col
    if waiting:
        named = count_table(listed_in(tail, leaf, list_rows, 1), first, table_rows)
        col = col + widened(named[0:chunks, :]) * refs[6][...]
    outs[1][...] = col


def add_block(list_rows, bits, left, tail, msg, totals, masked=True, waiting=(), row_type=jnp.float32):
    leaf = left.shape[0]
    nodes = lax.axis_size("node")
    part = (leaf, LANES)
    outs = [jax.ShapeDtypeStruct(part, row_type), jax.ShapeDtypeStruct(part, jnp.float32)]
    if not totals:
        table_shape = (-(-nodes * (leaf // LANES) // 8) * 8, LANES)
        outs.append(jax.ShapeDtypeStruct(table_shape, jnp.float32))
    result = pl.pallas_call(
        functools.partial(block_kernel, nodes, list_rows, bits, bool(totals), masked, len(waiting)),
        out_shape=outs,
        in_specs=[VMEM] * (3 + len(totals) + len(waiting)),
        out_specs=[VMEM] * len(outs),
        scratch_shapes=[pltpu.VMEM((32, leaf), jnp.bfloat16), pltpu.VMEM((leaf, leaf), jnp.bfloat16)],
        compiler_params=ROOM,
        name="add_block",
    )(left, tail, msg, *totals, *waiting)
    if not totals:
        return tuple(result), None
    if not masked:
        return (result[0], totals[1], totals[2]), result[1]
    return (result[0], result[1], totals[2]), None


def swap(block, axis, bits):
    return lax.ppermute(block, axis, [(i, i ^ bits) for i in range(lax.axis_size(axis))])


def on_device(coords, omega, skeleton):
    nodes = lax.axis_size("node")
    reps = lax.axis_size("rep")
    list_rows = reps * skeleton.shape[1] // LANES
    far_bits = [1 << k for k in range(2, nodes.bit_length() - 1)]

    across = [(0, omega)]
    for bit in reversed(far_bits):
        across += [(bits | bit, swap(block, "node", bit)) for bits, block in across]
    pieces = [swap(skeleton, "rep", bits) for bits in reversed(range(1, reps))]
    plain, left, own_piece = prep(coords, omega, skeleton)
    ahead = {step: swap(plain, "node", step) for step in (QUAD[0], QUAD[2])}
    msg, tail = attach(list_rows, plain, [own_piece] + pieces, coords.shape[1])
    tails = [(0, tail)]
    for bit in reversed(far_bits):
        tails += [(bits | bit, swap(part, "node", bit)) for bits, part in tails]
    group = {step: swap(msg, "node", step) for step in QUAD[1:2]}
    early, late = [], []
    for (bits, block), (_, part) in zip(across[1:], tails[1:]):
        packed = pack(list_rows, block, part, tail)
        sent = {}
        for step in (1, 3, 2):
            sent[step] = swap(packed, "node", step)
        late += [(bits, step, sent[step]) for step in (1, 3, 2)]
        early.append((bits, packed, True))
    early += [(step, block, True) for step, block in group.items()]
    totals, waiting = (), {}
    totals, _ = add_block(list_rows, 0, left, tail, msg, totals)
    for step, block in ahead.items():
        totals, left_over = add_block(list_rows, step, left, tail, block, totals, False)
        waiting[step] = (left_over,)
    for bits, block, masked in early:
        totals, _ = add_block(list_rows, bits, left, tail, block, totals, masked)
    for place, (bits, step, block) in enumerate(late):
        row_type = jnp.float32 if place + 1 < len(late) else jnp.bfloat16
        extra = waiting.pop(step, ())
        totals, _ = add_block(list_rows, bits | step, left, tail, block, totals, True, extra, row_type)
    return totals[:2]


def solution(mesh):
    in_specs = (P(None, "node"), P("node", "rep"), P("node", "rep"))
    out_specs = (P("node", "rep"), P("node", "rep"))
    return jax.shard_map(on_device, mesh=mesh, in_specs=in_specs, out_specs=out_specs, check_vma=False)
```

```python
import functools

import jax
import jax.numpy as jnp
from jax import lax
from jax.experimental import pallas as pl
from jax.experimental.pallas import tpu as pltpu
from jax.sharding import PartitionSpec as P


kernel_scale = 0.0078125
softening = 0.02
stretch = 1.0 / kernel_scale
soft_term = softening * softening * stretch * stretch
TERMS = 3
LANES = 128
BASE = 256
QUAD = (1, 2, 3)

VMEM = pl.BlockSpec(memory_space=pltpu.VMEM)
ROOM = pltpu.CompilerParams(vmem_limit_bytes=16 * 1024 * 1024)
FAST = pltpu.CompilerParams(vmem_limit_bytes=16 * 1024 * 1024)


def term_rows(leaf):
    return -(-4 * (leaf // LANES) // 16) * 16


def spare_row(leaf, index):
    chunks = leaf // LANES
    return (index // chunks) * term_rows(leaf) + 4 * (index % chunks) + 3


def split(value):
    terms = []
    for _ in range(TERMS):
        term = value.astype(jnp.bfloat16).astype(jnp.float32)
        value = value - term
        terms.append(term)
    return terms


def row_kind(rows):
    return lax.broadcasted_iota(jnp.int32, (rows, LANES), 0) % 4


def centred(points, nodes, me):
    kind = row_kind(points.shape[0])
    first = (2 * me + 1).astype(jnp.float32) * (stretch / nodes)
    middle = jnp.where(kind == 0, first, 0.5 * stretch)
    return jnp.where(kind == 3, 0.0, points - middle)


def factors(points, left):
    spare = row_kind(points.shape[0]) == 3
    square = points * points
    norm = pltpu.roll(square, 1, 0) + pltpu.roll(square, 2, 0) + pltpu.roll(square, 3, 0)
    norm = jnp.where(spare, norm + soft_term if left else norm, 0.0)
    one = jnp.where(spare, 1.0, 0.0)
    high, middle, low = split(-2.0 * points if left else points)
    norms = split(norm)
    if left:
        groups = [high + norms[0], high + norms[1], middle + norms[2], middle + one, high + one, low + one, middle, low]
    else:
        groups = [high + one, middle + one, high + one, middle + norms[0], low + norms[1], high + norms[2], low, middle]
    return groups


def chunk_of(groups, k):
    return jnp.concatenate([group[4 * k : 4 * k + 4, :] for group in groups], axis=0)


def prep_kernel(nodes, coords_ref, omega_ref, piece_ref, msg_ref, left_ref, own_ref, points, sems):
    leaf = points.shape[1]
    chunks = leaf // LANES
    fetch = pltpu.make_async_copy(coords_ref, points, sems.at[0])
    block = pltpu.make_async_copy(omega_ref, msg_ref.at[pl.ds(0, leaf)], sems.at[1])
    piece = pltpu.make_async_copy(piece_ref, own_ref, sems.at[2])
    fetch.start()
    block.start()
    piece.start()
    fetch.wait()
    scaled = points[...] * stretch
    blank = jnp.zeros((1, LANES), jnp.float32)
    rows = []
    for k in range(chunks):
        rows += [scaled[c : c + 1, k * LANES : (k + 1) * LANES] for c in range(3)] + [blank]
    rows += [blank] * (term_rows(leaf) - len(rows))
    rows = jnp.concatenate(rows, axis=0)
    msg_ref[leaf:, :] = jnp.concatenate(split(rows), axis=0).astype(jnp.bfloat16)
    groups = factors(centred(rows, nodes, lax.axis_index("node")), True)
    for k in range(chunks):
        left_ref[k * LANES : (k + 1) * LANES, :] = chunk_of(groups, k).T.astype(jnp.bfloat16)
    block.wait()
    piece.wait()


def prep(coords, omega, piece):
    leaf = coords.shape[1]
    operands = [pltpu.with_memory_space_constraint(x, pltpu.HBM) for x in (coords, omega, piece)]
    return pl.pallas_call(
        functools.partial(prep_kernel, lax.axis_size("node")),
        out_shape=(
            jax.ShapeDtypeStruct((leaf + TERMS * term_rows(leaf), LANES), jnp.bfloat16),
            jax.ShapeDtypeStruct((leaf, 32), jnp.bfloat16),
            jax.ShapeDtypeStruct(piece.shape, piece.dtype),
        ),
        in_specs=[pl.BlockSpec(memory_space=pltpu.HBM)] * 3,
        out_specs=(VMEM,) * 3,
        scratch_shapes=[pltpu.VMEM(coords.shape, jnp.float32), pltpu.SemaphoreType.DMA((3,))],
        compiler_params=ROOM,
        name="prep",
    )(*operands)


def attach_kernel(list_rows, msg_in_ref, *refs):
    pieces, msg_ref, tail_ref = refs[:-2], refs[-2], refs[-1]
    leaf = msg_ref.shape[0] - tail_ref.shape[0]
    listed = jnp.concatenate([piece[...] for piece in pieces], axis=1)
    tail = msg_in_ref[leaf:, :].astype(jnp.float32)
    place = lax.broadcasted_iota(jnp.int32, tail.shape, 0)
    index = 0
    for digit in (listed // BASE, listed % BASE):
        digit = digit.astype(jnp.float32)
        for r in range(list_rows):
            tail = jnp.where(place == spare_row(leaf, index), digit[:, r * LANES : (r + 1) * LANES], tail)
            index += 1
    tail = tail.astype(jnp.bfloat16)
    msg_ref[0:leaf, :] = msg_in_ref[0:leaf, :]
    msg_ref[leaf:, :] = tail
    tail_ref[...] = tail


def attach(list_rows, msg, pieces, leaf):
    return pl.pallas_call(
        functools.partial(attach_kernel, list_rows),
        out_shape=(
            jax.ShapeDtypeStruct(msg.shape, msg.dtype),
            jax.ShapeDtypeStruct((msg.shape[0] - leaf, LANES), msg.dtype),
        ),
        in_specs=[VMEM] * (1 + len(pieces)),
        out_specs=(VMEM, VMEM),
        compiler_params=ROOM,
        name="attach",
    )(msg, *pieces)


def pack_kernel(list_rows, block_ref, tail_ref, own_ref, msg_ref):
    leaf = block_ref.shape[0]
    msg_ref[0:leaf, :] = block_ref[...]
    tail, own = tail_ref[...].astype(jnp.float32), own_ref[...].astype(jnp.float32)
    place = lax.broadcasted_iota(jnp.int32, tail.shape, 0)
    for r in range(2 * list_rows):
        held = spare_row(leaf, r)
        tail = jnp.where(place == spare_row(leaf, 2 * list_rows + r), own[held : held + 1, :], tail)
    msg_ref[leaf:, :] = tail.astype(jnp.bfloat16)


def pack(list_rows, block, tail, own):
    return pl.pallas_call(
        functools.partial(pack_kernel, list_rows),
        out_shape=jax.ShapeDtypeStruct((block.shape[0] + tail.shape[0], LANES), block.dtype),
        in_specs=[VMEM] * 3,
        out_specs=VMEM,
        compiler_params=ROOM,
        name="pack",
    )(block, tail, own)


def listed_in(tail, leaf, list_rows, slot=0):
    places = [spare_row(leaf, 2 * list_rows * slot + r) for r in range(2 * list_rows)]
    digits = [tail[place : place + 1, :] for place in places]
    return [digits[r] * BASE + digits[list_rows + r] for r in range(list_rows)]


def count_table(listed, first, rows):
    total = jnp.zeros((rows, LANES), jnp.float32)
    for index in listed:
        row = jnp.floor(index * (1.0 / LANES))
        column = index - row * LANES
        rows_hit = jnp.where(lax.broadcasted_iota(jnp.int32, (rows, LANES), 0).astype(jnp.float32) + first == row, 1.0, 0.0)
        lanes_hit = jnp.where(lax.broadcasted_iota(jnp.int32, (LANES, LANES), 0).astype(jnp.float32) == column, 1.0, 0.0)
        total = total + lax.dot_general(
            rows_hit.astype(jnp.bfloat16),
            lanes_hit.astype(jnp.bfloat16),
            (((1,), (1,)), ((), ())),
            preferred_element_type=jnp.float32,
        )
    return total


def widened(table):
    rows = table.shape[0]
    if rows % 8:
        table = jnp.concatenate([table, jnp.zeros((8 - rows % 8, LANES), jnp.float32)], axis=0)
    columns = table.T
    return jnp.concatenate([jnp.broadcast_to(columns[:, k : k + 1], (LANES, LANES)) for k in range(rows)], axis=0)


def block_kernel(nodes, list_rows, bits, started, masked, waiting, *refs):
    left_ref, tail_ref, msg_ref = refs[:3]
    right_ref, tile_ref = refs[-2:]
    leaf = left_ref.shape[0]
    chunks = leaf // LANES
    me = lax.axis_index("node")
    first = (me * chunks).astype(jnp.float32)
    if started:
        row_in_ref, col_in_ref, table_ref = refs[3:6]
        outs = refs[6 + waiting : -2]
    else:
        outs = refs[3:-2]
        mine = listed_in(tail_ref[...].astype(jnp.float32), leaf, list_rows)
        table_ref = outs[2]
        table_ref[...] = count_table(mine, 0.0, table_ref.shape[0])
    tail = msg_ref[leaf:, :].astype(jnp.float32)
    term = term_rows(leaf)
    points = (tail[0:term, :] + tail[term : 2 * term, :]) + tail[2 * term : 3 * term, :]
    groups = factors(centred(points, nodes, me), False)
    for k in range(chunks):
        right_ref[:, k * LANES : (k + 1) * LANES] = chunk_of(groups, k).astype(jnp.bfloat16)
    for p in range(0, leaf, 2 * LANES):
        squared = jnp.dot(left_ref[...], right_ref[:, p : p + 2 * LANES], preferred_element_type=jnp.float32)
        tile_ref[:, p : p + 2 * LANES] = lax.rsqrt(squared).astype(jnp.bfloat16)
    node = me ^ bits
    near = jnp.where(jnp.abs(node - me) <= 1, 1.0, 0.0)
    samples = msg_ref[0:leaf, :]
    weight = widened(table_ref[pl.ds(node * chunks, chunks), :]) + near
    weighted = weight.astype(jnp.bfloat16) * samples
    both = jnp.dot(tile_ref[...], jnp.concatenate([samples, weighted], axis=1), preferred_element_type=jnp.float32)
    row, col = both[:, LANES:], both[:, :LANES]
    if started:
        row = row_in_ref[...] + row
    outs[0][...] = row.astype(outs[0].dtype)
    if not masked:
        outs[1][...] = col
        return
    table_rows = -(-chunks // 8) * 8
    named = count_table(listed_in(tail, leaf, list_rows), first, table_rows)
    col = widened(named[0:chunks, :]) * col
    if started:
        col = col_in_ref[...] + col
    if waiting:
        named = count_table(listed_in(tail, leaf, list_rows, 1), first, table_rows)
        col = col + widened(named[0:chunks, :]) * refs[6][...]
    outs[1][...] = col


def add_block(list_rows, bits, left, tail, msg, totals, masked=True, waiting=(), row_type=jnp.float32):
    leaf = left.shape[0]
    nodes = lax.axis_size("node")
    part = (leaf, LANES)
    outs = [jax.ShapeDtypeStruct(part, row_type), jax.ShapeDtypeStruct(part, jnp.float32)]
    if not totals:
        table_shape = (-(-nodes * (leaf // LANES) // 8) * 8, LANES)
        outs.append(jax.ShapeDtypeStruct(table_shape, jnp.float32))
    result = pl.pallas_call(
        functools.partial(block_kernel, nodes, list_rows, bits, bool(totals), masked, len(waiting)),
        out_shape=outs,
        in_specs=[VMEM] * (3 + len(totals) + len(waiting)),
        out_specs=[VMEM] * len(outs),
        scratch_shapes=[pltpu.VMEM((32, leaf), jnp.bfloat16), pltpu.VMEM((leaf, leaf), jnp.bfloat16)],
        compiler_params=FAST,
        name="add_block",
    )(left, tail, msg, *totals, *waiting)
    if not totals:
        return tuple(result), None
    if not masked:
        return (result[0], totals[1], totals[2]), result[1]
    return (result[0], result[1], totals[2]), None


def swap(block, axis, bits):
    return lax.ppermute(block, axis, [(i, i ^ bits) for i in range(lax.axis_size(axis))])


def on_device(coords, omega, skeleton):
    nodes = lax.axis_size("node")
    reps = lax.axis_size("rep")
    list_rows = reps * skeleton.shape[1] // LANES
    far_bits = [1 << k for k in range(2, nodes.bit_length() - 1)]

    across = [(0, omega)]
    for bit in reversed(far_bits):
        across += [(bits | bit, swap(block, "node", bit)) for bits, block in across]
    pieces = [swap(skeleton, "rep", bits) for bits in reversed(range(1, reps))]
    plain, left, own_piece = prep(coords, omega, skeleton)
    ahead = {step: swap(plain, "node", step) for step in (QUAD[0], QUAD[2])}
    msg, tail = attach(list_rows, plain, [own_piece] + pieces, coords.shape[1])
    tails = [(0, tail)]
    for bit in reversed(far_bits):
        tails += [(bits | bit, swap(part, "node", bit)) for bits, part in tails]
    group = {step: swap(msg, "node", step) for step in QUAD[1:2]}
    early, late = [], []
    for (bits, block), (_, part) in zip(across[1:], tails[1:]):
        packed = pack(list_rows, block, part, tail)
        sent = {}
        for step in (1, 3, 2):
            sent[step] = swap(packed, "node", step)
        late += [(bits, step, sent[step]) for step in (1, 3, 2)]
        early.append((bits, packed, True))
    early += [(step, block, True) for step, block in group.items()]
    totals, waiting = (), {}
    totals, _ = add_block(list_rows, 0, left, tail, msg, totals)
    for step, block in ahead.items():
        totals, left_over = add_block(list_rows, step, left, tail, block, totals, False)
        waiting[step] = (left_over,)
    for bits, block, masked in early:
        totals, _ = add_block(list_rows, bits, left, tail, block, totals, masked)
    for place, (bits, step, block) in enumerate(late):
        row_type = jnp.float32 if place + 1 < len(late) else jnp.bfloat16
        extra = waiting.pop(step, ())
        totals, _ = add_block(list_rows, bits | step, left, tail, block, totals, True, extra, row_type)
    return totals[:2]


def solution(mesh):
    in_specs = (P(None, "node"), P("node", "rep"), P("node", "rep"))
    out_specs = (P("node", "rep"), P("node", "rep"))
    return jax.shard_map(on_device, mesh=mesh, in_specs=in_specs, out_specs=out_specs, check_vma=False)
```

```python
import functools

import jax
import jax.numpy as jnp
from jax import lax
from jax.experimental import pallas as pl
from jax.experimental.pallas import tpu as pltpu
from jax.sharding import PartitionSpec as P


kernel_scale = 0.0078125
softening = 0.02
stretch = 1.0 / kernel_scale
soft_term = softening * softening * stretch * stretch
TERMS = 3
LANES = 128
DEPTH = 48
BASE = 256
QUAD = (1, 2, 3)

VMEM = pl.BlockSpec(memory_space=pltpu.VMEM)
ROOM = pltpu.CompilerParams(vmem_limit_bytes=16 * 1024 * 1024)
FAST = pltpu.CompilerParams(vmem_limit_bytes=16 * 1024 * 1024)


def term_rows(leaf):
    return -(-4 * (leaf // LANES) // 16) * 16


def spare_row(leaf, index):
    chunks = leaf // LANES
    return (index // chunks) * term_rows(leaf) + 4 * (index % chunks) + 3


def split(value):
    terms = []
    for _ in range(TERMS):
        term = value.astype(jnp.bfloat16).astype(jnp.float32)
        value = value - term
        terms.append(term)
    return terms


def row_kind(rows):
    return lax.broadcasted_iota(jnp.int32, (rows, LANES), 0) % 4


def centred(points, nodes, me):
    kind = row_kind(points.shape[0])
    first = (2 * me + 1).astype(jnp.float32) * (stretch / nodes)
    middle = jnp.where(kind == 0, first, 0.5 * stretch)
    return jnp.where(kind == 3, 0.0, points - middle)


def factors(points, left):
    spare = row_kind(points.shape[0]) == 3
    square = points * points
    norm = pltpu.roll(square, 1, 0) + pltpu.roll(square, 2, 0) + pltpu.roll(square, 3, 0)
    norm = jnp.where(spare, norm + soft_term if left else norm, 0.0)
    one = jnp.where(spare, 1.0, 0.0)
    high, middle, low = split(-2.0 * points if left else points)
    norms = split(norm)
    if left:
        groups = [high + norms[0], high + norms[1], middle + norms[2], middle + one, high + one, low + one]
        groups += [middle, low, low]
    else:
        groups = [high + one, middle + one, high + one, middle + norms[0], low + norms[1], high + norms[2]]
        groups += [low, middle, low]
    return groups + [jnp.zeros_like(points)] * (DEPTH // 4 - len(groups))


def chunk_of(groups, k):
    return jnp.concatenate([group[4 * k : 4 * k + 4, :] for group in groups], axis=0)


def prep_kernel(nodes, coords_ref, omega_ref, piece_ref, msg_ref, left_ref, own_ref, points, sems):
    leaf = points.shape[1]
    chunks = leaf // LANES
    fetch = pltpu.make_async_copy(coords_ref, points, sems.at[0])
    block = pltpu.make_async_copy(omega_ref, msg_ref.at[pl.ds(0, leaf)], sems.at[1])
    piece = pltpu.make_async_copy(piece_ref, own_ref, sems.at[2])
    fetch.start()
    block.start()
    piece.start()
    fetch.wait()
    scaled = points[...] * stretch
    blank = jnp.zeros((1, LANES), jnp.float32)
    rows = []
    for k in range(chunks):
        rows += [scaled[c : c + 1, k * LANES : (k + 1) * LANES] for c in range(3)] + [blank]
    rows += [blank] * (term_rows(leaf) - len(rows))
    rows = jnp.concatenate(rows, axis=0)
    msg_ref[leaf:, :] = jnp.concatenate(split(rows), axis=0).astype(jnp.bfloat16)
    groups = factors(centred(rows, nodes, lax.axis_index("node")), True)
    for k in range(chunks):
        left_ref[k * LANES : (k + 1) * LANES, :] = chunk_of(groups, k).T.astype(jnp.bfloat16)
    block.wait()
    piece.wait()


def prep(coords, omega, piece):
    leaf = coords.shape[1]
    operands = [pltpu.with_memory_space_constraint(x, pltpu.HBM) for x in (coords, omega, piece)]
    return pl.pallas_call(
        functools.partial(prep_kernel, lax.axis_size("node")),
        out_shape=(
            jax.ShapeDtypeStruct((leaf + TERMS * term_rows(leaf), LANES), jnp.bfloat16),
            jax.ShapeDtypeStruct((leaf, DEPTH), jnp.bfloat16),
            jax.ShapeDtypeStruct(piece.shape, piece.dtype),
        ),
        in_specs=[pl.BlockSpec(memory_space=pltpu.HBM)] * 3,
        out_specs=(VMEM,) * 3,
        scratch_shapes=[pltpu.VMEM(coords.shape, jnp.float32), pltpu.SemaphoreType.DMA((3,))],
        compiler_params=ROOM,
        name="prep",
    )(*operands)


def attach_kernel(list_rows, msg_in_ref, *refs):
    pieces, msg_ref, tail_ref = refs[:-2], refs[-2], refs[-1]
    leaf = msg_ref.shape[0] - tail_ref.shape[0]
    listed = jnp.concatenate([piece[...] for piece in pieces], axis=1)
    tail = msg_in_ref[leaf:, :].astype(jnp.float32)
    place = lax.broadcasted_iota(jnp.int32, tail.shape, 0)
    index = 0
    for digit in (listed // BASE, listed % BASE):
        digit = digit.astype(jnp.float32)
        for r in range(list_rows):
            tail = jnp.where(place == spare_row(leaf, index), digit[:, r * LANES : (r + 1) * LANES], tail)
            index += 1
    tail = tail.astype(jnp.bfloat16)
    msg_ref[0:leaf, :] = msg_in_ref[0:leaf, :]
    msg_ref[leaf:, :] = tail
    tail_ref[...] = tail


def attach(list_rows, msg, pieces, leaf):
    return pl.pallas_call(
        functools.partial(attach_kernel, list_rows),
        out_shape=(
            jax.ShapeDtypeStruct(msg.shape, msg.dtype),
            jax.ShapeDtypeStruct((msg.shape[0] - leaf, LANES), msg.dtype),
        ),
        in_specs=[VMEM] * (1 + len(pieces)),
        out_specs=(VMEM, VMEM),
        compiler_params=ROOM,
        name="attach",
    )(msg, *pieces)


def pack_kernel(list_rows, block_ref, tail_ref, own_ref, msg_ref):
    leaf = block_ref.shape[0]
    msg_ref[0:leaf, :] = block_ref[...]
    tail, own = tail_ref[...].astype(jnp.float32), own_ref[...].astype(jnp.float32)
    place = lax.broadcasted_iota(jnp.int32, tail.shape, 0)
    for r in range(2 * list_rows):
        held = spare_row(leaf, r)
        tail = jnp.where(place == spare_row(leaf, 2 * list_rows + r), own[held : held + 1, :], tail)
    msg_ref[leaf:, :] = tail.astype(jnp.bfloat16)


def pack(list_rows, block, tail, own):
    return pl.pallas_call(
        functools.partial(pack_kernel, list_rows),
        out_shape=jax.ShapeDtypeStruct((block.shape[0] + tail.shape[0], LANES), block.dtype),
        in_specs=[VMEM] * 3,
        out_specs=VMEM,
        compiler_params=ROOM,
        name="pack",
    )(block, tail, own)


def listed_in(tail, leaf, list_rows, slot=0):
    places = [spare_row(leaf, 2 * list_rows * slot + r) for r in range(2 * list_rows)]
    digits = [tail[place : place + 1, :] for place in places]
    return [digits[r] * BASE + digits[list_rows + r] for r in range(list_rows)]


def count_table(listed, first, rows):
    total = jnp.zeros((rows, LANES), jnp.float32)
    for index in listed:
        row = jnp.floor(index * (1.0 / LANES))
        column = index - row * LANES
        rows_hit = jnp.where(lax.broadcasted_iota(jnp.int32, (rows, LANES), 0).astype(jnp.float32) + first == row, 1.0, 0.0)
        lanes_hit = jnp.where(lax.broadcasted_iota(jnp.int32, (LANES, LANES), 0).astype(jnp.float32) == column, 1.0, 0.0)
        total = total + lax.dot_general(
            rows_hit.astype(jnp.bfloat16),
            lanes_hit.astype(jnp.bfloat16),
            (((1,), (1,)), ((), ())),
            preferred_element_type=jnp.float32,
        )
    return total


def widened(table):
    rows = table.shape[0]
    if rows % 8:
        table = jnp.concatenate([table, jnp.zeros((8 - rows % 8, LANES), jnp.float32)], axis=0)
    columns = table.T
    return jnp.concatenate([jnp.broadcast_to(columns[:, k : k + 1], (LANES, LANES)) for k in range(rows)], axis=0)


def block_kernel(nodes, list_rows, bits, started, masked, waiting, *refs):
    left_ref, tail_ref, msg_ref = refs[:3]
    right_ref, tile_ref = refs[-2:]
    leaf = left_ref.shape[0]
    chunks = leaf // LANES
    me = lax.axis_index("node")
    first = (me * chunks).astype(jnp.float32)
    if started:
        row_in_ref, col_in_ref, table_ref = refs[3:6]
        outs = refs[6 + waiting : -2]
    else:
        outs = refs[3:-2]
        mine = listed_in(tail_ref[...].astype(jnp.float32), leaf, list_rows)
        table_ref = outs[2]
        table_ref[...] = count_table(mine, 0.0, table_ref.shape[0])
    tail = msg_ref[leaf:, :].astype(jnp.float32)
    term = term_rows(leaf)
    points = (tail[0:term, :] + tail[term : 2 * term, :]) + tail[2 * term : 3 * term, :]
    groups = factors(centred(points, nodes, me), False)
    for k in range(chunks):
        right_ref[:, k * LANES : (k + 1) * LANES] = chunk_of(groups, k).astype(jnp.bfloat16)
    for p in range(0, leaf, 2 * LANES):
        squared = jnp.dot(left_ref[...], right_ref[:, p : p + 2 * LANES], preferred_element_type=jnp.float32)
        tile_ref[:, p : p + 2 * LANES] = lax.rsqrt(squared).astype(jnp.bfloat16)
    node = me ^ bits
    near = jnp.where(jnp.abs(node - me) <= 1, 1.0, 0.0)
    samples = msg_ref[0:leaf, :]
    weight = widened(table_ref[pl.ds(node * chunks, chunks), :]) + near
    weighted = weight.astype(jnp.bfloat16) * samples
    both = jnp.dot(tile_ref[...], jnp.concatenate([samples, weighted], axis=1), preferred_element_type=jnp.float32)
    row, col = both[:, LANES:], both[:, :LANES]
    if started:
        row = row_in_ref[...] + row
    outs[0][...] = row.astype(outs[0].dtype)
    if not masked:
        outs[1][...] = col
        return
    table_rows = -(-chunks // 8) * 8
    named = count_table(listed_in(tail, leaf, list_rows), first, table_rows)
    col = widened(named[0:chunks, :]) * col
    if started:
        col = col_in_ref[...] + col
    if waiting:
        named = count_table(listed_in(tail, leaf, list_rows, 1), first, table_rows)
        col = col + widened(named[0:chunks, :]) * refs[6][...]
    outs[1][...] = col


def add_block(list_rows, bits, left, tail, msg, totals, masked=True, waiting=(), row_type=jnp.float32):
    leaf = left.shape[0]
    nodes = lax.axis_size("node")
    part = (leaf, LANES)
    outs = [jax.ShapeDtypeStruct(part, row_type), jax.ShapeDtypeStruct(part, jnp.float32)]
    if not totals:
        table_shape = (-(-nodes * (leaf // LANES) // 8) * 8, LANES)
        outs.append(jax.ShapeDtypeStruct(table_shape, jnp.float32))
    result = pl.pallas_call(
        functools.partial(block_kernel, nodes, list_rows, bits, bool(totals), masked, len(waiting)),
        out_shape=outs,
        in_specs=[VMEM] * (3 + len(totals) + len(waiting)),
        out_specs=[VMEM] * len(outs),
        scratch_shapes=[pltpu.VMEM((DEPTH, leaf), jnp.bfloat16), pltpu.VMEM((leaf, leaf), jnp.bfloat16)],
        compiler_params=FAST,
        name="add_block",
    )(left, tail, msg, *totals, *waiting)
    if not totals:
        return tuple(result), None
    if not masked:
        return (result[0], totals[1], totals[2]), result[1]
    return (result[0], result[1], totals[2]), None


def swap(block, axis, bits):
    return lax.ppermute(block, axis, [(i, i ^ bits) for i in range(lax.axis_size(axis))])


def on_device(coords, omega, skeleton):
    nodes = lax.axis_size("node")
    reps = lax.axis_size("rep")
    list_rows = reps * skeleton.shape[1] // LANES
    far_bits = [1 << k for k in range(2, nodes.bit_length() - 1)]

    across = [(0, omega)]
    for bit in reversed(far_bits):
        across += [(bits | bit, swap(block, "node", bit)) for bits, block in across]
    pieces = [swap(skeleton, "rep", bits) for bits in reversed(range(1, reps))]
    plain, left, own_piece = prep(coords, omega, skeleton)
    ahead = {step: swap(plain, "node", step) for step in (QUAD[0], QUAD[2])}
    msg, tail = attach(list_rows, plain, [own_piece] + pieces, coords.shape[1])
    tails = [(0, tail)]
    for bit in reversed(far_bits):
        tails += [(bits | bit, swap(part, "node", bit)) for bits, part in tails]
    group = {step: swap(msg, "node", step) for step in QUAD[1:2]}
    early, late = [], []
    for (bits, block), (_, part) in zip(across[1:], tails[1:]):
        packed = pack(list_rows, block, part, tail)
        sent = {}
        for step in (1, 3, 2):
            sent[step] = swap(packed, "node", step)
        late += [(bits, step, sent[step]) for step in (1, 3, 2)]
        early.append((bits, packed, True))
    early += [(step, block, True) for step, block in group.items()]
    totals, waiting = (), {}
    totals, _ = add_block(list_rows, 0, left, tail, msg, totals)
    for step, block in ahead.items():
        totals, left_over = add_block(list_rows, step, left, tail, block, totals, False)
        waiting[step] = (left_over,)
    for bits, block, masked in early:
        totals, _ = add_block(list_rows, bits, left, tail, block, totals, masked)
    for place, (bits, step, block) in enumerate(late):
        row_type = jnp.float32 if place + 1 < len(late) else jnp.bfloat16
        extra = waiting.pop(step, ())
        totals, _ = add_block(list_rows, bits | step, left, tail, block, totals, True, extra, row_type)
    return totals[:2]


def solution(mesh):
    in_specs = (P(None, "node"), P("node", "rep"), P("node", "rep"))
    out_specs = (P("node", "rep"), P("node", "rep"))
    return jax.shard_map(on_device, mesh=mesh, in_specs=in_specs, out_specs=out_specs, check_vma=False)
```

```python
import functools

import jax
import jax.numpy as jnp
from jax import lax
from jax.experimental import pallas as pl
from jax.experimental.pallas import tpu as pltpu
from jax.sharding import PartitionSpec as P


kernel_scale = 0.0078125
softening = 0.02
stretch = 1.0 / kernel_scale
soft_term = softening * softening * stretch * stretch
TERMS = 3
LANES = 128
DEPTH = 48
BASE = 256
QUAD = (1, 2, 3)

VMEM = pl.BlockSpec(memory_space=pltpu.VMEM)
ROOM = pltpu.CompilerParams(vmem_limit_bytes=16 * 1024 * 1024)
FAST = pltpu.CompilerParams(vmem_limit_bytes=16 * 1024 * 1024)


def term_rows(leaf):
    return -(-4 * (leaf // LANES) // 16) * 16


def spare_row(leaf, index):
    chunks = leaf // LANES
    return (index // chunks) * term_rows(leaf) + 4 * (index % chunks) + 3


def split(value):
    terms = []
    for _ in range(TERMS):
        term = value.astype(jnp.bfloat16).astype(jnp.float32)
        value = value - term
        terms.append(term)
    return terms


def row_kind(rows):
    return lax.broadcasted_iota(jnp.int32, (rows, LANES), 0) % 4


def centred(points, nodes, me):
    kind = row_kind(points.shape[0])
    first = (2 * me + 1).astype(jnp.float32) * (stretch / nodes)
    middle = jnp.where(kind == 0, first, 0.5 * stretch)
    return jnp.where(kind == 3, 0.0, points - middle)


def factors(points, left):
    spare = row_kind(points.shape[0]) == 3
    square = points * points
    norm = pltpu.roll(square, 1, 0) + pltpu.roll(square, 2, 0) + pltpu.roll(square, 3, 0)
    norm = jnp.where(spare, norm + soft_term if left else norm, 0.0)
    one = jnp.where(spare, 1.0, 0.0)
    high, middle, low = split(-2.0 * points if left else points)
    norms = split(norm)
    if left:
        groups = [high + norms[0], high + norms[1], middle + norms[2], middle + one, high + one, low + one]
        groups += [middle, low, low]
    else:
        groups = [high + one, middle + one, high + one, middle + norms[0], low + norms[1], high + norms[2]]
        groups += [low, middle, low]
    return groups + [jnp.zeros_like(points)] * (DEPTH // 4 - len(groups))


def chunk_of(groups, k):
    return jnp.concatenate([group[4 * k : 4 * k + 4, :] for group in groups], axis=0)


def prep_kernel(nodes, coords_ref, omega_ref, piece_ref, msg_ref, left_ref, own_ref, points, sems):
    leaf = points.shape[1]
    chunks = leaf // LANES
    fetch = pltpu.make_async_copy(coords_ref, points, sems.at[0])
    block = pltpu.make_async_copy(omega_ref, msg_ref.at[pl.ds(0, leaf)], sems.at[1])
    piece = pltpu.make_async_copy(piece_ref, own_ref, sems.at[2])
    fetch.start()
    block.start()
    piece.start()
    fetch.wait()
    scaled = points[...] * stretch
    blank = jnp.zeros((1, LANES), jnp.float32)
    rows = []
    for k in range(chunks):
        rows += [scaled[c : c + 1, k * LANES : (k + 1) * LANES] for c in range(3)] + [blank]
    rows += [blank] * (term_rows(leaf) - len(rows))
    rows = jnp.concatenate(rows, axis=0)
    msg_ref[leaf:, :] = jnp.concatenate(split(rows), axis=0).astype(jnp.bfloat16)
    groups = factors(centred(rows, nodes, lax.axis_index("node")), True)
    for k in range(chunks):
        left_ref[k * LANES : (k + 1) * LANES, :] = chunk_of(groups, k).T.astype(jnp.bfloat16)
    block.wait()
    piece.wait()


def prep(coords, omega, piece):
    leaf = coords.shape[1]
    operands = [pltpu.with_memory_space_constraint(x, pltpu.HBM) for x in (coords, omega, piece)]
    return pl.pallas_call(
        functools.partial(prep_kernel, lax.axis_size("node")),
        out_shape=(
            jax.ShapeDtypeStruct((leaf + TERMS * term_rows(leaf), LANES), jnp.bfloat16),
            jax.ShapeDtypeStruct((leaf, DEPTH), jnp.bfloat16),
            jax.ShapeDtypeStruct(piece.shape, piece.dtype),
        ),
        in_specs=[pl.BlockSpec(memory_space=pltpu.HBM)] * 3,
        out_specs=(VMEM,) * 3,
        scratch_shapes=[pltpu.VMEM(coords.shape, jnp.float32), pltpu.SemaphoreType.DMA((3,))],
        compiler_params=ROOM,
        name="prep",
    )(*operands)


def attach_kernel(list_rows, msg_in_ref, *refs):
    pieces, msg_ref, tail_ref = refs[:-2], refs[-2], refs[-1]
    leaf = msg_ref.shape[0] - tail_ref.shape[0]
    listed = jnp.concatenate([piece[...] for piece in pieces], axis=1)
    tail = msg_in_ref[leaf:, :].astype(jnp.float32)
    place = lax.broadcasted_iota(jnp.int32, tail.shape, 0)
    index = 0
    for digit in (listed // BASE, listed % BASE):
        digit = digit.astype(jnp.float32)
        for r in range(list_rows):
            tail = jnp.where(place == spare_row(leaf, index), digit[:, r * LANES : (r + 1) * LANES], tail)
            index += 1
    tail = tail.astype(jnp.bfloat16)
    msg_ref[0:leaf, :] = msg_in_ref[0:leaf, :]
    msg_ref[leaf:, :] = tail
    tail_ref[...] = tail


def attach(list_rows, msg, pieces, leaf):
    return pl.pallas_call(
        functools.partial(attach_kernel, list_rows),
        out_shape=(
            jax.ShapeDtypeStruct(msg.shape, msg.dtype),
            jax.ShapeDtypeStruct((msg.shape[0] - leaf, LANES), msg.dtype),
        ),
        in_specs=[VMEM] * (1 + len(pieces)),
        out_specs=(VMEM, VMEM),
        compiler_params=ROOM,
        name="attach",
    )(msg, *pieces)


def pack_kernel(list_rows, block_ref, tail_ref, own_ref, msg_ref):
    leaf = block_ref.shape[0]
    msg_ref[0:leaf, :] = block_ref[...]
    tail, own = tail_ref[...].astype(jnp.float32), own_ref[...].astype(jnp.float32)
    place = lax.broadcasted_iota(jnp.int32, tail.shape, 0)
    for r in range(2 * list_rows):
        held = spare_row(leaf, r)
        tail = jnp.where(place == spare_row(leaf, 2 * list_rows + r), own[held : held + 1, :], tail)
    msg_ref[leaf:, :] = tail.astype(jnp.bfloat16)


def pack(list_rows, block, tail, own):
    return pl.pallas_call(
        functools.partial(pack_kernel, list_rows),
        out_shape=jax.ShapeDtypeStruct((block.shape[0] + tail.shape[0], LANES), block.dtype),
        in_specs=[VMEM] * 3,
        out_specs=VMEM,
        compiler_params=ROOM,
        name="pack",
    )(block, tail, own)


def listed_in(tail, leaf, list_rows, slot=0):
    places = [spare_row(leaf, 2 * list_rows * slot + r) for r in range(2 * list_rows)]
    digits = [tail[place : place + 1, :] for place in places]
    return [digits[r] * BASE + digits[list_rows + r] for r in range(list_rows)]


def count_table(listed, first, rows):
    total = jnp.zeros((rows, LANES), jnp.float32)
    for index in listed:
        row = jnp.floor(index * (1.0 / LANES))
        column = index - row * LANES
        rows_hit = jnp.where(lax.broadcasted_iota(jnp.int32, (rows, LANES), 0).astype(jnp.float32) + first == row, 1.0, 0.0)
        lanes_hit = jnp.where(lax.broadcasted_iota(jnp.int32, (LANES, LANES), 0).astype(jnp.float32) == column, 1.0, 0.0)
        total = total + lax.dot_general(
            rows_hit.astype(jnp.bfloat16),
            lanes_hit.astype(jnp.bfloat16),
            (((1,), (1,)), ((), ())),
            preferred_element_type=jnp.float32,
        )
    return total


def widened(table):
    rows = table.shape[0]
    if rows % 8:
        table = jnp.concatenate([table, jnp.zeros((8 - rows % 8, LANES), jnp.float32)], axis=0)
    columns = table.T
    return jnp.concatenate([jnp.broadcast_to(columns[:, k : k + 1], (LANES, LANES)) for k in range(rows)], axis=0)


def block_kernel(nodes, list_rows, bits, started, masked, waiting, *refs):
    left_ref, tail_ref, msg_ref = refs[:3]
    right_ref, tile_ref = refs[-2:]
    leaf = left_ref.shape[0]
    chunks = leaf // LANES
    me = lax.axis_index("node")
    first = (me * chunks).astype(jnp.float32)
    if started:
        row_in_ref, col_in_ref, table_ref = refs[3:6]
        outs = refs[6 + waiting : -2]
    else:
        outs = refs[3:-2]
        mine = listed_in(tail_ref[...].astype(jnp.float32), leaf, list_rows)
        table_ref = outs[2]
        table_ref[...] = count_table(mine, 0.0, table_ref.shape[0])
    tail = msg_ref[leaf:, :].astype(jnp.float32)
    table_rows = -(-chunks // 8) * 8
    masks = []
    for slot in range((1 + waiting) * masked):
        named = count_table(listed_in(tail, leaf, list_rows, slot), first, table_rows)
        masks.append(widened(named[0:chunks, :]))
    term = term_rows(leaf)
    points = (tail[0:term, :] + tail[term : 2 * term, :]) + tail[2 * term : 3 * term, :]
    groups = factors(centred(points, nodes, me), False)
    for k in range(chunks):
        right_ref[:, k * LANES : (k + 1) * LANES] = chunk_of(groups, k).astype(jnp.bfloat16)
    for p in range(0, leaf, 2 * LANES):
        squared = jnp.dot(left_ref[...], right_ref[:, p : p + 2 * LANES], preferred_element_type=jnp.float32)
        tile_ref[:, p : p + 2 * LANES] = lax.rsqrt(squared).astype(jnp.bfloat16)
    node = me ^ bits
    near = jnp.where(jnp.abs(node - me) <= 1, 1.0, 0.0)
    samples = msg_ref[0:leaf, :]
    weight = widened(table_ref[pl.ds(node * chunks, chunks), :]) + near
    weighted = weight.astype(jnp.bfloat16) * samples
    both = jnp.dot(tile_ref[...], jnp.concatenate([samples, weighted], axis=1), preferred_element_type=jnp.float32)
    row, col = both[:, LANES:], both[:, :LANES]
    if started:
        row = row_in_ref[...] + row
    outs[0][...] = row.astype(outs[0].dtype)
    if not masked:
        outs[1][...] = col
        return
    col = masks[0] * col
    if started:
        col = col_in_ref[...] + col
    if waiting:
        col = col + masks[1] * refs[6][...]
    outs[1][...] = col


def add_block(list_rows, bits, left, tail, msg, totals, masked=True, waiting=(), row_type=jnp.float32):
    leaf = left.shape[0]
    nodes = lax.axis_size("node")
    part = (leaf, LANES)
    outs = [jax.ShapeDtypeStruct(part, row_type), jax.ShapeDtypeStruct(part, jnp.float32)]
    if not totals:
        table_shape = (-(-nodes * (leaf // LANES) // 8) * 8, LANES)
        outs.append(jax.ShapeDtypeStruct(table_shape, jnp.float32))
    result = pl.pallas_call(
        functools.partial(block_kernel, nodes, list_rows, bits, bool(totals), masked, len(waiting)),
        out_shape=outs,
        in_specs=[VMEM] * (3 + len(totals) + len(waiting)),
        out_specs=[VMEM] * len(outs),
        scratch_shapes=[pltpu.VMEM((DEPTH, leaf), jnp.bfloat16), pltpu.VMEM((leaf, leaf), jnp.bfloat16)],
        compiler_params=FAST,
        name="add_block",
    )(left, tail, msg, *totals, *waiting)
    if not totals:
        return tuple(result), None
    if not masked:
        return (result[0], totals[1], totals[2]), result[1]
    return (result[0], result[1], totals[2]), None


def swap(block, axis, bits):
    return lax.ppermute(block, axis, [(i, i ^ bits) for i in range(lax.axis_size(axis))])


def on_device(coords, omega, skeleton):
    nodes = lax.axis_size("node")
    reps = lax.axis_size("rep")
    list_rows = reps * skeleton.shape[1] // LANES
    far_bits = [1 << k for k in range(2, nodes.bit_length() - 1)]

    across = [(0, omega)]
    for bit in reversed(far_bits):
        across += [(bits | bit, swap(block, "node", bit)) for bits, block in across]
    pieces = [swap(skeleton, "rep", bits) for bits in reversed(range(1, reps))]
    plain, left, own_piece = prep(coords, omega, skeleton)
    ahead = {step: swap(plain, "node", step) for step in (QUAD[0], QUAD[2])}
    msg, tail = attach(list_rows, plain, [own_piece] + pieces, coords.shape[1])
    tails = [(0, tail)]
    for bit in reversed(far_bits):
        tails += [(bits | bit, swap(part, "node", bit)) for bits, part in tails]
    group = {step: swap(msg, "node", step) for step in QUAD[1:2]}
    early, late = [], []
    for (bits, block), (_, part) in zip(across[1:], tails[1:]):
        packed = pack(list_rows, block, part, tail)
        sent = {}
        for step in (1, 3, 2):
            sent[step] = swap(packed, "node", step)
        late += [(bits, step, sent[step]) for step in (1, 3, 2)]
        early.append((bits, packed, True))
    early += [(step, block, True) for step, block in group.items()]
    totals, waiting = (), {}
    totals, _ = add_block(list_rows, 0, left, tail, msg, totals)
    for step, block in ahead.items():
        totals, left_over = add_block(list_rows, step, left, tail, block, totals, False)
        waiting[step] = (left_over,)
    for bits, block, masked in early:
        totals, _ = add_block(list_rows, bits, left, tail, block, totals, masked)
    for place, (bits, step, block) in enumerate(late):
        row_type = jnp.float32 if place + 1 < len(late) else jnp.bfloat16
        extra = waiting.pop(step, ())
        totals, _ = add_block(list_rows, bits | step, left, tail, block, totals, True, extra, row_type)
    return totals[:2]


def solution(mesh):
    in_specs = (P(None, "node"), P("node", "rep"), P("node", "rep"))
    out_specs = (P("node", "rep"), P("node", "rep"))
    return jax.shard_map(on_device, mesh=mesh, in_specs=in_specs, out_specs=out_specs, check_vma=False)
```
